256 devices in a mesh: grp: 8 (over z), shard: 32 (over y, x, core).
Axes of the slice: x: 4, y: 4, z: 8, core: 2. Of those that a mesh axis runs over, the one named last changes fastest.
Arguments:
- table: float32 [4096, 8, 128], P('shard')
- table_first: float32 [4096, 8, 128], P('shard'), may hold values from -3 to 3
- table_second: float32 [4096, 8, 128], P('shard')
- slot_table: int32 [4096], P('shard'), may hold values from 0 to 25
- touched: int32 [8, 4096], P('grp', 'shard'), may hold values from 0 to 4095, as said below
- emb_grads: bfloat16 [8, 4096, 8, 128], P('grp', 'shard'), may hold values from -6 to 6
- block_slot: int32 [4096], replicated, may hold values from 0 to 4095, as said below
- dense_x: bfloat16 [13, 1048576], P(None, ('grp', 'shard')), may hold values from -6 to 6
- dense_cot: bfloat16 [1048576, 128], P(('grp', 'shard')), may hold values from -0.0625 to 0.0625
- w_one: float32 [13, 512], replicated, may hold values from -1.75 to 1.75
- w_two: float32 [512, 256], replicated, may hold values from -0.25 to 0.25
- w_three: float32 [256, 128], replicated, may hold values from -0.375 to 0.375
- first_one: float32 [13, 512], replicated, may hold values from -3 to 3
- first_two: float32 [512, 256], replicated, may hold values from -3 to 3
- first_three: float32 [256, 128], replicated, may hold values from -3 to 3
- second_one: float32 [13, 512], replicated, may hold values from 0.001 to 0.3
- second_two: float32 [512, 256], replicated, may hold values from 0.001 to 0.3
- second_three: float32 [256, 128], replicated, may hold values from 0.001 to 0.3
Outputs:
- new_table: float32 [4096, 8, 128], P('shard')
- new_table_first: float32 [4096, 8, 128], P('shard')
- new_table_second: float32 [4096, 8, 128], P('shard')
- new_w_one: float32 [13, 512], replicated
- new_w_two: float32 [512, 256], replicated
- new_w_three: float32 [256, 128], replicated
- new_first_one: float32 [13, 512], replicated
- new_first_two: float32 [512, 256], replicated
- new_first_three: float32 [256, 128], replicated
- new_second_one: float32 [13, 512], replicated
- new_second_two: float32 [512, 256], replicated
- new_second_three: float32 [256, 128], replicated
The draws below stay inside these ranges and needn't reach their ends.
Inputs may be any that keep to these rules, and one draw needn't show every extreme that they name: `touched`: each device's 128 ids are distinct; at most 8 of them have block_slot // 128 equal to any one shard, and in every draw some shard gets exactly 8 from every device. `block_slot`: A permutation of the 4096 slots.
All inputs are finite; a program needn't handle non-finite values.
Results may differ from the reference program's by a relative error of at most 0.0037.
Values may be sent and summed in bfloat16 or wider, within the bound.
No kernel may reach another device: no remote copies, remote signals or barrier semaphores. Data moves between devices by JAX's collectives and lax.ppermute only.
A program may use at most 128 MiB of HBM per device.

```python
import math
import jax
import jax.numpy as jnp
from jax import lax

E = 128
DIN = 13
H1 = 512
H2 = 256
TABLES = 26
BLK = 8
CAP = 8
NB_DEV = 128
TOK_DEV = 4096
K = 128
NB = 4096
TOKENS = 1048576
N_GRP = 8
N_SHARD = 32


def common_slots(key):
    forward = jax.random.permutation(jax.random.fold_in(key, 11), NB).astype(jnp.int32)
    inverse = jnp.zeros((NB,), jnp.int32).at[forward].set(jnp.arange(NB, dtype=jnp.int32))
    return (forward, inverse)


def draw_block_slot(key, part):
    return common_slots(key)[0]


def draw_touched(key, part):
    forward, inverse = common_slots(key)
    devices_all = N_GRP * N_SHARD
    candidates = N_SHARD * CAP
    live_count = max(CAP, NB_DEV * 5 // 8)
    hottest = jax.random.randint(jax.random.fold_in(key, 12), (), 0, N_SHARD)
    owner_bias = jax.random.randint(jax.random.fold_in(key, 13), (devices_all, N_SHARD), 0, 4)
    owner_bias = jnp.where(jnp.arange(N_SHARD)[None, :] == hottest, 8, owner_bias)
    noise_keys = jax.random.split(jax.random.fold_in(key, 14), devices_all)
    noise = jax.vmap(lambda subkey: jax.random.permutation(subkey, candidates))(noise_keys).astype(jnp.int32)
    cand_owner = jnp.arange(candidates, dtype=jnp.int32) // CAP
    scores = owner_bias[:, cand_owner] * 1048576 + noise
    unused, chosen = lax.top_k(scores, K)
    owner_keys = jax.random.split(jax.random.fold_in(key, 17), N_SHARD)
    live_sets = jax.vmap(lambda subkey: jax.random.permutation(subkey, NB_DEV)[:live_count])(owner_keys).astype(jnp.int32)
    row_keys = jax.random.split(jax.random.fold_in(key, 15), devices_all * N_SHARD)
    live_pick = jax.vmap(lambda subkey: jax.random.permutation(subkey, live_count)[:CAP])(row_keys).astype(jnp.int32)
    live_pick = live_pick.reshape(devices_all, N_SHARD, CAP)
    owner_rows = jnp.arange(N_SHARD, dtype=jnp.int32)[None, :, None]
    local_rows = live_sets[owner_rows, live_pick].reshape(devices_all, candidates)
    local_pick = jnp.take_along_axis(local_rows, chosen, axis=1)
    slot_pick = chosen // CAP * NB_DEV + local_pick
    block_ids = inverse[slot_pick]
    order_keys = jax.random.split(jax.random.fold_in(key, 16), devices_all)
    orders = jax.vmap(lambda subkey: jax.random.permutation(subkey, K))(order_keys).astype(jnp.int32)
    block_ids = jnp.take_along_axis(block_ids, orders, axis=1)
    return block_ids.reshape(N_GRP, N_SHARD * K).astype(jnp.int32)


def slot_rise():
    slot_pos = jnp.arange(NB, dtype=jnp.float32)
    return 1.0 + 2.0 * slot_pos / max(NB - 1, 1)


def draw_table(key, part):
    rise = slot_rise()
    row_scale = 10.0 ** jax.random.uniform(jax.random.fold_in(key, 21), (NB, BLK, 1), jnp.float32)
    col_scale = 10.0 ** (jax.random.uniform(jax.random.fold_in(key, 22), (1, 1, E), jnp.float32) - 1.0)
    base = jax.random.normal(jax.random.fold_in(key, 23), (NB, BLK, E), jnp.float32)
    return (base * row_scale * col_scale * rise[:, None, None]).astype(jnp.float32)


def draw_table_second(key, part):
    rise = slot_rise()
    expo = jax.random.uniform(jax.random.fold_in(key, 31), (NB, BLK, E), jnp.float32, -3.0, -0.5)
    return (10.0 ** expo / (rise * rise)[:, None, None]).astype(jnp.float32)


def place_ends(drawn, rng, smallest, largest):
    dims = drawn.shape
    place = [jax.random.randint(jax.random.fold_in(rng, axis), (), 0, dims[axis]) for axis in range(len(dims))]
    drawn = drawn.at[tuple(place)].set(smallest)
    longest = dims.index(max(dims))
    place[longest] = (place[longest] + 1) % dims[longest]
    return drawn.at[tuple(place)].set(largest)


def levels(key, shape, cuts, low, top_value):
    loudness = 1.0
    for position, blocks in cuts:
        heights = jax.random.uniform(jax.random.fold_in(jax.random.fold_in(key, 6), position), (blocks,), jnp.float32, low / len(cuts), top_value / len(cuts))
        loudness = loudness * jnp.repeat(jnp.exp(heights), shape[position] // blocks).reshape((-1,) + (1,) * (len(shape) - 1 - position))
    return loudness


def gaussian(own_key, extent, width, most, cuts=(), kind=jnp.bfloat16):
    gain = levels(own_key, extent, cuts, -0.22, 0.18) if cuts else 1.0
    entries = jax.random.normal(own_key, extent, jnp.float32) * width * gain
    return jnp.minimum(jnp.maximum(entries, -most), most).astype(kind)


def setup_inputs(seed: int = 0) -> dict:
    keys = jax.random.split(jax.random.key(seed), 19)
    return {
        "table": draw_table(jax.random.fold_in(keys[18], 71), 0),
        "table_first": gaussian(keys[1], (NB, BLK, E), 0.2, 3.0, ((0, 32),), jnp.float32),
        "table_second": draw_table_second(jax.random.fold_in(keys[18], 71), 0),
        "slot_table": place_ends(jax.random.randint(keys[3], (NB,), 0, TABLES), jax.random.fold_in(keys[3], 1), 0, TABLES - 1).astype(jnp.int32),
        "touched": draw_touched(jax.random.fold_in(keys[18], 71), 0),
        "emb_grads": gaussian(keys[5], (N_GRP, N_SHARD * K, BLK, E), 1.0, 6.0, ((0, 8), (1, 32))),
        "block_slot": draw_block_slot(jax.random.fold_in(keys[18], 71), 0),
        "dense_x": gaussian(keys[7], (DIN, TOKENS), 1.0, 6.0, ((1, 256),)),
        "dense_cot": gaussian(keys[8], (TOKENS, E), (4 * TOKENS ** -0.5), 0.0625, ((0, 256),)),
        "w_one": gaussian(keys[9], (DIN, H1), DIN ** -0.5, 1.75, (), jnp.float32),
        "w_two": gaussian(keys[10], (H1, H2), H1 ** -0.5, 0.25, (), jnp.float32),
        "w_three": gaussian(keys[11], (H2, E), H2 ** -0.5, 0.375, (), jnp.float32),
        "first_one": gaussian(keys[12], (DIN, H1), 0.2, 3.0, (), jnp.float32),
        "first_two": gaussian(keys[13], (H1, H2), 0.2, 3.0, (), jnp.float32),
        "first_three": gaussian(keys[14], (H2, E), 0.2, 3.0, (), jnp.float32),
        "second_one": jnp.clip(jnp.exp(jax.random.uniform(keys[15], (DIN, H1), jnp.float32, math.log(0.001), math.log(0.3))), 0.001, 0.3),
        "second_two": jnp.clip(jnp.exp(jax.random.uniform(keys[16], (H1, H2), jnp.float32, math.log(0.001), math.log(0.3))), 0.001, 0.3),
        "second_three": jnp.clip(jnp.exp(jax.random.uniform(keys[17], (H2, E), jnp.float32, math.log(0.001), math.log(0.3))), 0.001, 0.3),
    }


beta_one = 0.9
beta_two = 0.999
corr_first = 1.0 - 0.9 ** 10
corr_second = 1.0 - 0.999 ** 10
adam_eps = 1e-06
decay_rate = 0.01
learn_rate = 0.1
ratio_eps = 1e-06

def silu_slope(pre_value):
    logistic = jax.nn.sigmoid(pre_value)
    return logistic * (1.0 + pre_value * (1.0 - logistic))

def tower_grads(dense_x, dense_cot, w_one, w_two, w_three):
    w_one_bf = w_one.astype(jnp.bfloat16)
    w_two_bf = w_two.astype(jnp.bfloat16)
    w_three_bf = w_three.astype(jnp.bfloat16)
    pre_one = lax.dot_general(dense_x, w_one_bf, (((0,), (0,)), ((), ())), preferred_element_type=jnp.float32)
    hidden_one = jax.nn.silu(pre_one).astype(jnp.bfloat16)
    pre_two = jnp.dot(hidden_one, w_two_bf, preferred_element_type=jnp.float32)
    hidden_two = jax.nn.silu(pre_two).astype(jnp.bfloat16)
    grad_three = lax.dot_general(hidden_two, dense_cot, (((0,), (0,)), ((), ())), preferred_element_type=jnp.float32)
    back_two = (lax.dot_general(dense_cot, w_three_bf, (((1,), (1,)), ((), ())), preferred_element_type=jnp.float32) * silu_slope(pre_two)).astype(jnp.bfloat16)
    grad_two = lax.dot_general(hidden_one, back_two, (((0,), (0,)), ((), ())), preferred_element_type=jnp.float32)
    back_one = (lax.dot_general(back_two, w_two_bf, (((1,), (1,)), ((), ())), preferred_element_type=jnp.float32) * silu_slope(pre_one)).astype(jnp.bfloat16)
    grad_one = jnp.dot(dense_x, back_one, preferred_element_type=jnp.float32)
    return (grad_one, grad_two, grad_three)

def lamb_dense(weight, first_in, second_in, gradient):
    first_out = beta_one * first_in + (1.0 - beta_one) * gradient
    second_out = beta_two * second_in + (1.0 - beta_two) * gradient * gradient
    update = first_out / corr_first / (jnp.sqrt(second_out / corr_second) + adam_eps) + decay_rate * weight
    trust_ratio = jnp.sqrt(jnp.sum(weight * weight)) / (jnp.sqrt(jnp.sum(update * update)) + ratio_eps)
    return (weight - learn_rate * trust_ratio * update, first_out, second_out)

def reference(table, table_first, table_second, slot_table, touched, emb_grads, block_slot, dense_x, dense_cot, w_one, w_two, w_three, first_one, first_two, first_three, second_one, second_two, second_three):
    slot_index = block_slot[touched].reshape(-1)
    flat_grads = emb_grads.reshape(-1, BLK, E).astype(jnp.float32)
    emb_grad = jnp.zeros((NB, BLK, E), jnp.float32).at[slot_index].add(flat_grads)
    hits = jnp.zeros((NB,), jnp.float32).at[slot_index].add(jnp.ones(slot_index.shape, jnp.float32))
    touched_mask = (hits > 0.5)[:, None, None]
    new_first = jnp.where(touched_mask, beta_one * table_first + (1.0 - beta_one) * emb_grad, table_first)
    new_second = jnp.where(touched_mask, beta_two * table_second + (1.0 - beta_two) * emb_grad * emb_grad, table_second)
    update = jnp.where(touched_mask, new_first / corr_first / (jnp.sqrt(new_second / corr_second) + adam_eps) + decay_rate * table, 0.0)
    weight_sq = jax.ops.segment_sum(lax.optimization_barrier(jnp.sum(table * table, axis=(1, 2))), slot_table, TABLES)
    update_sq = jax.ops.segment_sum(lax.optimization_barrier(jnp.sum(update * update, axis=(1, 2))), slot_table, TABLES)
    table_ratio = jnp.sqrt(weight_sq) / (jnp.sqrt(update_sq) + ratio_eps)
    new_table = table - learn_rate * table_ratio[slot_table][:, None, None] * update
    blocks_all = N_GRP * N_SHARD
    x_blocks = dense_x.reshape(DIN, blocks_all, TOK_DEV).transpose(1, 0, 2)
    cot_blocks = dense_cot.reshape(blocks_all, TOK_DEV, E)

    def accumulate(totals, inputs):
        terms = tower_grads(inputs[0], inputs[1], w_one, w_two, w_three)
        return ((totals[0] + terms[0], totals[1] + terms[1], totals[2] + terms[2]), None)
    start_sums = (jnp.zeros((DIN, H1), jnp.float32), jnp.zeros((H1, H2), jnp.float32), jnp.zeros((H2, E), jnp.float32))
    grads, unused = lax.scan(accumulate, start_sums, (x_blocks, cot_blocks))
    layer_one = lamb_dense(w_one, first_one, second_one, grads[0])
    layer_two = lamb_dense(w_two, first_two, second_two, grads[1])
    layer_three = lamb_dense(w_three, first_three, second_three, grads[2])
    return (new_table, new_first, new_second, layer_one[0], layer_two[0], layer_three[0], layer_one[1], layer_two[1], layer_three[1], layer_one[2], layer_two[2], layer_three[2])
```

```python
import functools
import jax
import jax.numpy as jnp
from jax import lax
from jax.experimental import pallas as pl
from jax.experimental.pallas import tpu as pltpu
from jax.sharding import Mesh
from jax.sharding import PartitionSpec as P

TABLES = 26
CAP = 8
SHARD = ("shard_0", "shard_1", "shard_2")
GRP_SHARD = ("grp", "shard_0", "shard_1", "shard_2")
SUB = 8
LANE = 128

beta_one = 0.9
beta_two = 0.999
corr_first = 1.0 - 0.9**10
corr_second = 1.0 - 0.999**10
adam_eps = 1e-06
decay_rate = 0.01
learn_rate = 0.1
ratio_eps = 1e-06

f32 = jnp.float32
bf16 = jnp.bfloat16
VMEM = pl.BlockSpec(memory_space=pltpu.VMEM)
SMEM = pl.BlockSpec(memory_space=pltpu.SMEM)


def lanes():
    return lax.broadcasted_iota(jnp.int32, (SUB, LANE), 1)


def subs():
    return lax.broadcasted_iota(jnp.int32, (SUB, LANE), 0)


def bucket_kernel(shards, blocks, ids, block_slot, grads, out, count, local):
    width = CAP + 1
    out[...] = jnp.zeros_like(out)
    for s in range(shards):
        count[s] = 0
    for r in range(shards * CAP):
        local[r] = 0

    def place(i, carry):
        slot = block_slot[ids[0, i]]
        owner = slot // blocks
        rank = count[owner]
        count[owner] = rank + 1
        out[owner * width + rank] = grads[i]
        local[owner * CAP + rank] = slot - owner * blocks + 1
        return carry

    lax.fori_loop(0, grads.shape[0], place, 0, unroll=8)
    lane = lanes()
    for s in range(shards):
        tile = jnp.zeros((SUB, LANE), f32)
        for a in range(CAP):
            tile = jnp.where(lane == a, local[s * CAP + a].astype(f32), tile)
        out[s * width + CAP] = tile.astype(bf16)


def bucketed(touched, block_slot, grads, shards, blocks):
    return pl.pallas_call(
        functools.partial(bucket_kernel, shards, blocks),
        out_shape=jax.ShapeDtypeStruct((shards * (CAP + 1), SUB, LANE), bf16),
        in_specs=[SMEM, SMEM, VMEM],
        out_specs=VMEM,
        scratch_shapes=[
            pltpu.SMEM((shards,), jnp.int32),
            pltpu.SMEM((shards * CAP,), jnp.int32),
        ],
        name="bucket",
    )(touched, block_slot, grads)


def combine_kernel(shards, groups, blocks, recv, out, total, place_v, place_s, hit, sem):
    width = CAP + 1
    own = blocks // groups
    for s in range(shards):
        place_v[s : s + 1, :] = recv[s * width + CAP].astype(f32)[0:1, :].astype(jnp.int32)
    copy = pltpu.make_async_copy(place_v, place_s, sem)
    copy.start()
    total[...] = jnp.zeros_like(total)
    for q in range(blocks + 1):
        hit[q] = 0
    copy.wait()

    def add(s, carry):
        for a in range(CAP):
            slot = place_s[s, a]
            total[slot] = total[slot] + recv[s * width + a].astype(f32)
            hit[slot] = 1
        return carry

    lax.fori_loop(0, shards, add, 0)
    lane = lanes()
    for g in range(groups):
        out[g * (own + 1) : g * (own + 1) + own] = total[1 + g * own : 1 + (g + 1) * own].astype(
            bf16
        )
        tile = jnp.zeros((SUB, LANE), f32)
        for j in range(own):
            tile = jnp.where(lane == j, hit[1 + g * own + j].astype(f32), tile)
        out[g * (own + 1) + own] = tile.astype(bf16)


def combined(recv, shards, groups, blocks):
    own = blocks // groups
    return pl.pallas_call(
        functools.partial(combine_kernel, shards, groups, blocks),
        out_shape=jax.ShapeDtypeStruct((groups * (own + 1), SUB, LANE), bf16),
        in_specs=[VMEM],
        out_specs=VMEM,
        scratch_shapes=[
            pltpu.VMEM((blocks + 1, SUB, LANE), f32),
            pltpu.VMEM((shards, LANE), jnp.int32),
            pltpu.SMEM((shards, LANE), jnp.int32),
            pltpu.SMEM((blocks + 1,), jnp.int32),
            pltpu.SemaphoreType.DMA,
        ],
        name="combine",
    )(recv)


def act(pre):
    gate = 0.5 * jnp.tanh(0.5 * pre) + 0.5
    hidden = pre * gate
    return hidden.astype(bf16), gate + hidden * (1.0 - gate)


def dot(a, b, ca, cb):
    return lax.dot_general(a, b, (((ca,), (cb,)), ((), ())), preferred_element_type=f32)


def tower_kernel(shards, x, cot, w_one_t, w_two, w_two_t, w_three, out, g_one, g_two, g_three):
    step = pl.program_id(0)

    @pl.when(step == 0)
    def _():
        g_one[...] = jnp.zeros_like(g_one)
        g_two[...] = jnp.zeros_like(g_two)
        g_three[...] = jnp.zeros_like(g_three)

    xs = x[...]
    cots = cot[...]
    hidden_one, slope_one = act(dot(w_one_t[...], xs, 1, 0))
    hidden_two, slope_two = act(dot(w_two_t[...], hidden_one, 1, 0))
    g_three[...] += dot(hidden_two, cots, 1, 0)
    back_two = (dot(w_three[...], cots, 1, 1) * slope_two).astype(bf16)
    g_two[...] += dot(hidden_one, back_two, 1, 1)
    back_one = (dot(w_two[...], back_two, 1, 0) * slope_one).astype(bf16)
    g_one[0 : xs.shape[0], :] += dot(xs, back_one, 1, 1)

    @pl.when(step == pl.num_programs(0) - 1)
    def _():
        rows_two = g_two.shape[0] // shards
        rows_three = g_three.shape[0] // shards
        halves = g_two.shape[1] // LANE
        for s in range(shards):
            at = 0
            for h in range(halves):
                for r in range(0, rows_two, SUB):
                    out[s, at] = g_two[
                        s * rows_two + r : s * rows_two + r + SUB, h * LANE : (h + 1) * LANE
                    ].astype(bf16)
                    at += 1
            for r in range(0, rows_three, SUB):
                out[s, at] = g_three[s * rows_three + r : s * rows_three + r + SUB, :].astype(bf16)
                at += 1
            c, r = s // 2, s % 2
            if c < g_one.shape[1] // LANE:
                out[s, at] = g_one[r * SUB : (r + 1) * SUB, c * LANE : (c + 1) * LANE].astype(bf16)
            else:
                out[s, at] = jnp.zeros((SUB, LANE), bf16)


def tower(x, cot, w_one, w_two, w_three, shards, tiles, step=512):
    din, samples = x.shape
    h_one, h_two = w_two.shape
    width = w_three.shape[1]
    whole = lambda shape: pl.BlockSpec(shape, lambda i: tuple(0 for _ in shape))
    macs = samples * (2 * din * h_one + 3 * h_one * h_two + 2 * h_two * width)
    return pl.pallas_call(
        functools.partial(tower_kernel, shards),
        grid=(samples // step,),
        out_shape=jax.ShapeDtypeStruct((shards, tiles, SUB, LANE), bf16),
        in_specs=[
            pl.BlockSpec((din, step), lambda i: (0, i)),
            pl.BlockSpec((step, width), lambda i: (i, 0)),
            whole((h_one, din)),
            whole((h_one, h_two)),
            whole((h_two, h_one)),
            whole((h_two, width)),
        ],
        out_specs=whole((shards, tiles, SUB, LANE)),
        scratch_shapes=[
            pltpu.VMEM((2 * SUB, h_one), f32),
            pltpu.VMEM((h_one, h_two), f32),
            pltpu.VMEM((h_two, width), f32),
        ],
        cost_estimate=pl.CostEstimate(
            flops=2 * macs, bytes_accessed=4 * samples * width, transcendentals=samples * h_one
        ),
        name="tower",
    )(
        x,
        cot,
        w_one.T.astype(bf16),
        w_two.astype(bf16),
        w_two.T.astype(bf16),
        w_three.astype(bf16),
    )


def lamb_step(weight, first_in, second_in, gradient):
    first_out = beta_one * first_in + (1.0 - beta_one) * gradient
    second_out = beta_two * second_in + (1.0 - beta_two) * gradient * gradient
    update = (
        first_out / corr_first / (jnp.sqrt(second_out / corr_second) + adam_eps)
        + decay_rate * weight
    )
    return update, first_out, second_out


def flags_of(tile, own):
    return [jnp.broadcast_to(tile[0:1, j : j + 1], (SUB, LANE)) > 0.5 for j in range(own)]


def split_rows(rows):
    tile = jnp.zeros((SUB, LANE), f32)
    sub = subs()
    for i, row in enumerate(rows):
        high = row.astype(bf16).astype(f32)
        tile = jnp.where(sub == 2 * i, high, tile)
        tile = jnp.where(sub == 2 * i + 1, row - high, tile)
    return tile.astype(bf16)


def own_kernel(groups, shards, tiles, who, slot_table, recv, dense, table, first, second, out):
    own = out.shape[1] - 2 - tiles
    at = who[0] * own
    rows = recv[0:own].astype(f32)
    flag = recv[own].astype(f32)
    for g in range(1, groups):
        rows = rows + recv[g * (own + 1) : g * (own + 1) + own].astype(f32)
        flag = flag + recv[g * (own + 1) + own].astype(f32)
    sent = rows.astype(bf16)
    touched = flags_of(flag, own)
    lane = lax.broadcasted_iota(jnp.int32, (1, LANE), 1)
    weight_sq = jnp.zeros((1, LANE), f32)
    update_sq = jnp.zeros((1, LANE), f32)
    for j in range(own):
        weight = table[at + j]
        update, unused, unused_too = lamb_step(
            weight, first[at + j], second[at + j], sent[j].astype(f32)
        )
        update = jnp.where(touched[j], update, 0.0)
        mine = lane == slot_table[at + j]
        weight_sq += jnp.where(mine, jnp.sum(weight * weight, keepdims=True), 0.0)
        update_sq += jnp.where(mine, jnp.sum(update * update, keepdims=True), 0.0)
    sums = dense[0].astype(f32)
    for s in range(1, shards):
        sums = sums + dense[s].astype(f32)
    sums = sums.astype(bf16)
    flag = flag.astype(bf16)
    both = split_rows((weight_sq, update_sq))
    for g in range(groups):
        out[g, 0:own] = sent
        out[g, own] = flag
        out[g, own + 1] = both
        out[g, own + 2 :] = sums


def owned(who, slot_table, recv, dense, table, first, second, groups, shards, tiles):
    own = table.shape[0] // groups
    return pl.pallas_call(
        functools.partial(own_kernel, groups, shards, tiles),
        out_shape=jax.ShapeDtypeStruct((groups, own + 2 + tiles, SUB, LANE), bf16),
        in_specs=[SMEM, SMEM] + [VMEM] * 5,
        out_specs=VMEM,
        name="own",
    )(who, slot_table, recv, dense, table, first, second)


def pack_kernel(groups, own, recv, out):
    dense = recv[0, own + 2 :].astype(f32)
    both = recv[0, own + 1].astype(f32)
    for g in range(1, groups):
        dense = dense + recv[g, own + 2 :].astype(f32)
        both = both + recv[g, own + 1].astype(f32)
    dense = dense.astype(bf16)
    both = split_rows((both[0:1] + both[1:2], both[2:3] + both[3:4]))
    for s in range(out.shape[0]):
        out[s, 0:-1] = dense
        out[s, out.shape[1] - 1] = both


def packed(recv, groups, shards, own, tiles):
    return pl.pallas_call(
        functools.partial(pack_kernel, groups, own),
        out_shape=jax.ShapeDtypeStruct((shards, tiles + 1, SUB, LANE), bf16),
        in_specs=[VMEM],
        out_specs=VMEM,
        name="pack",
    )(recv)


def slots_kernel(groups, own, recv, table, first, second, new_first, new_second, update_out):
    for g in range(groups):
        touched = flags_of(recv[g, own].astype(f32), own)
        for j in range(own):
            q = g * own + j
            update, first_out, second_out = lamb_step(
                table[q], first[q], second[q], recv[g, j].astype(f32)
            )
            new_first[q] = jnp.where(touched[j], first_out, first[q])
            new_second[q] = jnp.where(touched[j], second_out, second[q])
            update_out[q] = jnp.where(touched[j], update, 0.0)


def slots(recv, table, first, second, groups, own):
    shape = jax.ShapeDtypeStruct(table.shape, f32)
    return pl.pallas_call(
        functools.partial(slots_kernel, groups, own),
        out_shape=(shape,) * 3,
        in_specs=[VMEM] * 4,
        out_specs=(VMEM,) * 3,
        cost_estimate=pl.CostEstimate(
            flops=2000 * table.size, bytes_accessed=24 * table.size, transcendentals=table.size
        ),
        name="slots",
    )(recv, table, first, second)


def lamb_whole(weight, first_in, second_in, gradient):
    update, first_out, second_out = lamb_step(weight, first_in, second_in, gradient)
    ratio = jnp.sqrt(jnp.sum(weight * weight, keepdims=True)) / (
        jnp.sqrt(jnp.sum(update * update, keepdims=True)) + ratio_eps
    )
    return (weight - learn_rate * ratio * update, first_out, second_out)


def last_kernel(
    shards,
    slot_table,
    recv,
    table,
    update,
    w_one,
    w_two,
    w_three,
    first_one,
    first_two,
    first_three,
    second_one,
    second_two,
    second_three,
    new_table,
    new_w_one,
    new_w_two,
    new_w_three,
    new_first_one,
    new_first_two,
    new_first_three,
    new_second_one,
    new_second_two,
    new_second_three,
    ratio_v,
    ratio_s,
    g_one,
    g_two,
    g_three,
    sem,
):
    tiles = recv.shape[1] - 1
    both = recv[0, tiles].astype(f32)
    for s in range(1, shards):
        both = both + recv[s, tiles].astype(f32)
    weight_sq = both[0:1] + both[1:2]
    update_sq = both[2:3] + both[3:4]
    ratio = learn_rate * (jnp.sqrt(weight_sq) / (jnp.sqrt(update_sq) + ratio_eps))
    ratio_v[...] = jnp.broadcast_to(ratio, (SUB, LANE))
    copy = pltpu.make_async_copy(ratio_v, ratio_s, sem)
    copy.start()
    rows_two = g_two.shape[0] // shards
    rows_three = g_three.shape[0] // shards
    halves = g_two.shape[1] // LANE
    for s in range(shards):
        at = 0
        for h in range(halves):
            for r in range(0, rows_two, SUB):
                g_two[s * rows_two + r : s * rows_two + r + SUB, h * LANE : (h + 1) * LANE] = recv[
                    s, at
                ].astype(f32)
                at += 1
        for r in range(0, rows_three, SUB):
            g_three[s * rows_three + r : s * rows_three + r + SUB, :] = recv[s, at].astype(f32)
            at += 1
        c, r = s // 2, s % 2
        if c < g_one.shape[1] // LANE:
            g_one[r * SUB : (r + 1) * SUB, c * LANE : (c + 1) * LANE] = recv[s, at].astype(f32)
    for w, f, v, g, nw, nf, nv in (
        (w_one, first_one, second_one, g_one, new_w_one, new_first_one, new_second_one),
        (w_two, first_two, second_two, g_two, new_w_two, new_first_two, new_second_two),
        (w_three, first_three, second_three, g_three, new_w_three, new_first_three, new_second_three),
    ):
        nw[...], nf[...], nv[...] = lamb_whole(w[...], f[...], v[...], g[0 : w.shape[0], :])
    copy.wait()

    def step(q, carry):
        new_table[q] = table[q] - ratio_s[0, slot_table[q]] * update[q]
        return carry

    lax.fori_loop(0, table.shape[0], step, 0, unroll=8)


def last(slot_table, recv, table, update, weights, shards):
    outs = (table,) + weights
    return pl.pallas_call(
        functools.partial(last_kernel, shards),
        out_shape=tuple(jax.ShapeDtypeStruct(a.shape, f32) for a in outs),
        in_specs=[SMEM] + [VMEM] * 12,
        out_specs=(VMEM,) * 10,
        scratch_shapes=[
            pltpu.VMEM((SUB, LANE), f32),
            pltpu.SMEM((SUB, LANE), f32),
            pltpu.VMEM((2 * SUB, weights[0].shape[1]), f32),
            pltpu.VMEM(weights[1].shape, f32),
            pltpu.VMEM(weights[2].shape, f32),
            pltpu.SemaphoreType.DMA,
        ],
        name="last",
    )(slot_table, recv, table, update, *weights)


def exchange(value, axis):
    return lax.all_to_all(value, axis, split_axis=0, concat_axis=0, tiled=True)


def body(
    table,
    table_first,
    table_second,
    slot_table,
    touched,
    emb_grads,
    block_slot,
    dense_x,
    dense_cot,
    w_one,
    w_two,
    w_three,
    first_one,
    first_two,
    first_three,
    second_one,
    second_two,
    second_three,
):
    shards = lax.axis_size(SHARD)
    groups = lax.axis_size("grp")
    blocks = table.shape[0]
    own = blocks // groups
    tiles = (w_two.size + w_three.size) // (shards * SUB * LANE) + 1
    who = jnp.reshape(lax.axis_index("grp"), (1,)).astype(jnp.int32)

    send = bucketed(touched, block_slot, emb_grads[0], shards, blocks)
    recv = exchange(send.reshape(shards, CAP + 1, SUB, LANE), SHARD)
    dense = tower(dense_x, dense_cot, w_one, w_two, w_three, shards, tiles)
    part = combined(recv.reshape(send.shape), shards, groups, blocks)
    dense = exchange(dense, SHARD)
    part = exchange(part.reshape(groups, own + 1, SUB, LANE), "grp")
    mine = owned(
        who,
        slot_table,
        part.reshape(-1, SUB, LANE),
        dense,
        table,
        table_first,
        table_second,
        groups,
        shards,
        tiles,
    )
    whole = exchange(mine, "grp")
    spread = exchange(packed(whole, groups, shards, own, tiles), SHARD)
    new_first, new_second, update = slots(whole, table, table_first, table_second, groups, own)
    weights = (
        w_one,
        w_two,
        w_three,
        first_one,
        first_two,
        first_three,
        second_one,
        second_two,
        second_three,
    )
    new_table, *rest = last(slot_table, spread, table, update, weights, shards)
    return (new_table, new_first, new_second, *rest)


def solution(mesh):
    finer = Mesh(
        mesh.devices.reshape(mesh.shape["grp"], 4, 4, 2), ("grp", "shard_0", "shard_1", "shard_2")
    )
    rows = P(SHARD, None, None)
    placed = (
        rows,
        rows,
        rows,
        P(SHARD),
        P("grp", SHARD),
        P("grp", SHARD, None, None),
        P(),
        P(None, GRP_SHARD),
        P(GRP_SHARD, None),
    ) + (P(),) * 9
    return jax.shard_map(
        body,
        mesh=finer,
        in_specs=placed,
        out_specs=(rows, rows, rows) + (P(),) * 9,
        check_vma=False,
    )
```

```python
import functools
import jax
import jax.numpy as jnp
from jax import lax
from jax.experimental import pallas as pl
from jax.experimental.pallas import tpu as pltpu
from jax.sharding import Mesh
from jax.sharding import PartitionSpec as P

TABLES = 26
CAP = 8
SHARD = ("shard_0", "shard_1", "shard_2")
GRP_SHARD = ("grp", "shard_0", "shard_1", "shard_2")
SUB = 8
LANE = 128

beta_one = 0.9
beta_two = 0.999
corr_first = 1.0 - 0.9**10
corr_second = 1.0 - 0.999**10
adam_eps = 1e-06
decay_rate = 0.01
learn_rate = 0.1
ratio_eps = 1e-06

f32 = jnp.float32
bf16 = jnp.bfloat16
VMEM = pl.BlockSpec(memory_space=pltpu.VMEM)
SMEM = pl.BlockSpec(memory_space=pltpu.SMEM)


LIMIT = pltpu.CompilerParams(vmem_limit_bytes=20 * 2**20)


def iota(shape, dim):
    return lax.broadcasted_iota(jnp.int32, shape, dim)


def subs():
    return iota((SUB, LANE), 0)


def dot(a, b, ca, cb):
    return lax.dot_general(a, b, (((ca,), (cb,)), ((), ())), preferred_element_type=f32)


def log_two(n):
    return n.bit_length() - 1


def route_kernel(shards, blocks, groups, ids, block_slot, grads, out, wide):
    count = ids.shape[1]
    wide[...] = grads[...].astype(f32)
    for g in range(groups):
        rows = wide[pl.ds(g, count, stride=groups), :]
        out[g, 0 : count // SUB] = rows.reshape(count // SUB, SUB, LANE).astype(bf16)
    table_rows = block_slot.shape[0]
    high = ids[...] >> log_two(LANE)
    low = ids[...] & (LANE - 1)
    high_hot = iota((table_rows, count), 0) == high
    low_hot = iota((LANE, count), 0) == low
    slot = block_slot[...]
    one = high_hot.astype(f32).astype(bf16)
    owner_of = (slot >> log_two(blocks)).astype(f32).astype(bf16)
    local_of = (slot & (blocks - 1)).astype(f32).astype(bf16)
    owner = jnp.sum(jnp.where(low_hot, dot(owner_of, one, 0, 0), 0.0), axis=0, keepdims=True)
    local = jnp.sum(jnp.where(low_hot, dot(local_of, one, 0, 0), 0.0), axis=0, keepdims=True)
    owner_hot = iota((shards, count), 0).astype(f32) == owner
    before = (iota((count, count), 0) < iota((count, count), 1)).astype(f32).astype(bf16)
    rank = dot(owner_hot.astype(f32).astype(bf16), before, 1, 0)
    rank = jnp.sum(jnp.where(owner_hot, rank, 0.0), axis=0, keepdims=True)
    sub = iota((SUB, count), 0)
    tile = jnp.where(sub == 0, owner * CAP + rank, jnp.where(sub == 1, local + 1.0, 0.0))
    tile = tile.astype(bf16)
    for g in range(groups):
        out[g, count // SUB] = tile


def routed(ids, block_slot, grads, shards, blocks, groups):
    count = ids.shape[1]
    return pl.pallas_call(
        functools.partial(route_kernel, shards, blocks, groups),
        out_shape=jax.ShapeDtypeStruct((groups, count // SUB + 1, SUB, LANE), bf16),
        in_specs=[VMEM] * 3,
        out_specs=VMEM,
        scratch_shapes=[pltpu.VMEM(grads.shape, f32)],
        compiler_params=LIMIT,
        name="route",
    )(ids, block_slot, grads)


def bucket_kernel(shards, who, recv, dense, out):
    groups = recv.shape[0]
    tiles = dense.shape[1]
    count = LANE
    local_rows = jnp.zeros((shards, LANE), f32)
    for g in range(groups):
        tile = recv[g, count // SUB].astype(f32)
        place = tile[0:1].astype(jnp.int32)
        picker = (iota((shards * CAP, count), 0) == place).astype(f32).astype(bf16)
        rows = recv[g, 0 : count // SUB].astype(f32).reshape(count, LANE).astype(bf16)
        out[:, g] = dot(picker, rows, 1, 0).reshape(shards, SUB, LANE).astype(bf16)
        owner = place >> log_two(CAP)
        lane = (place & (CAP - 1)) + g * CAP + who[2] * (LANE // 2)
        local = jnp.where(iota((shards, count), 0) == owner, tile[1:2], 0.0).astype(bf16)
        spot = (iota((LANE, count), 0) == lane).astype(f32).astype(bf16)
        local_rows += dot(local, spot, 1, 1)
    sub = subs()
    for s in range(shards):
        out[s, groups : groups + tiles - 1] = dense[s, 0 : tiles - 1]
        tile = dense[s, tiles - 1].astype(f32)
        tile = jnp.where(sub == meta_row(s), local_rows[s : s + 1], tile)
        out[s, groups + tiles - 1] = tile.astype(bf16)


def meta_row(s):
    return (2 * (s % 4) + 2) % SUB


def bucketed(who, recv, dense):
    shards, tiles = dense.shape[:2]
    return pl.pallas_call(
        functools.partial(bucket_kernel, shards),
        out_shape=jax.ShapeDtypeStruct((shards, recv.shape[0] + tiles, SUB, LANE), bf16),
        in_specs=[SMEM, VMEM, VMEM],
        out_specs=VMEM,
        compiler_params=LIMIT,
        name="bucket",
    )(who, recv, dense)


def act(pre):
    gate = 0.5 * jnp.tanh(0.5 * pre) + 0.5
    hidden = pre * gate
    return hidden.astype(bf16), gate + hidden * (1.0 - gate)


def tower_kernel(
    shards, x, cot, w_one_in, w_two_in, w_three_in, out, g_one, g_two, g_three, w_two, w_two_t
):
    step = pl.program_id(0)

    @pl.when(step == 0)
    def _():
        g_one[...] = jnp.zeros_like(g_one)
        g_two[...] = jnp.zeros_like(g_two)
        g_three[...] = jnp.zeros_like(g_three)
        w_two[...] = w_two_in[...].astype(bf16)
        w_two_t[...] = w_two_in[...].T.astype(bf16)

    xs = x[...]
    cots = cot[...]
    hidden_one, slope_one = act(dot(w_one_in[...].astype(bf16), xs, 0, 0))
    hidden_two, slope_two = act(dot(w_two_t[...], hidden_one, 1, 0))
    g_three[...] += dot(hidden_two, cots, 1, 0)
    back_two = (dot(w_three_in[...].astype(bf16), cots, 1, 1) * slope_two).astype(bf16)
    g_two[...] += dot(hidden_one, back_two, 1, 1)
    back_one = (dot(w_two[...], back_two, 1, 0) * slope_one).astype(bf16)
    g_one[0 : xs.shape[0], :] += dot(xs, back_one, 1, 1)

    @pl.when(step == pl.num_programs(0) - 1)
    def _():
        rows_two = g_two.shape[0] // shards
        rows_three = g_three.shape[0] // shards
        halves = g_two.shape[1] // LANE
        for s in range(shards):
            at = 0
            for h in range(halves):
                for r in range(0, rows_two, SUB):
                    out[s, at] = g_two[
                        s * rows_two + r : s * rows_two + r + SUB, h * LANE : (h + 1) * LANE
                    ].astype(bf16)
                    at += 1
            for r in range(0, rows_three, SUB):
                out[s, at] = g_three[s * rows_three + r : s * rows_three + r + SUB, :].astype(bf16)
                at += 1
            c, r = s // 4 // 2, s // 4 % 2
            out[s, at] = g_one[r * SUB : (r + 1) * SUB, c * LANE : (c + 1) * LANE].astype(bf16)


def tower(x, cot, w_one, w_two, w_three, shards, tiles, step=512):
    din, samples = x.shape
    h_one, h_two = w_two.shape
    width = w_three.shape[1]
    whole = lambda shape: pl.BlockSpec(shape, lambda i: tuple(0 for _ in shape))
    macs = samples * (2 * din * h_one + 3 * h_one * h_two + 2 * h_two * width)
    return pl.pallas_call(
        functools.partial(tower_kernel, shards),
        grid=(samples // step,),
        out_shape=jax.ShapeDtypeStruct((shards, tiles, SUB, LANE), bf16),
        in_specs=[
            pl.BlockSpec((din, step), lambda i: (0, i)),
            pl.BlockSpec((step, width), lambda i: (i, 0)),
            whole((din, h_one)),
            whole((h_one, h_two)),
            whole((h_two, width)),
        ],
        out_specs=whole((shards, tiles, SUB, LANE)),
        scratch_shapes=[
            pltpu.VMEM((2 * SUB, h_one), f32),
            pltpu.VMEM((h_one, h_two), f32),
            pltpu.VMEM((h_two, width), f32),
            pltpu.VMEM((h_one, h_two), bf16),
            pltpu.VMEM((h_two, h_one), bf16),
        ],
        compiler_params=LIMIT,
        cost_estimate=pl.CostEstimate(
            flops=2 * macs, bytes_accessed=4 * samples * width, transcendentals=samples * h_one
        ),
        name="tower",
    )(x, cot, w_one, w_two, w_three)


def lamb_step(weight, first_in, second_in, gradient):
    first_out = beta_one * first_in + (1.0 - beta_one) * gradient
    second_out = beta_two * second_in + (1.0 - beta_two) * gradient * gradient
    update = (
        first_out / corr_first / (jnp.sqrt(second_out / corr_second) + adam_eps)
        + decay_rate * weight
    )
    return update, first_out, second_out


def split_rows(rows):
    tile = jnp.zeros((SUB, LANE), f32)
    sub = subs()
    for i, row in enumerate(rows):
        high = row.astype(bf16).astype(f32)
        tile = jnp.where(sub == 2 * i, high, tile)
        tile = jnp.where(sub == 2 * i + 1, row - high, tile)
    return tile.astype(bf16)


def table_hot(slot_table):
    return slot_table[...] == iota((slot_table.shape[0], LANE), 1)


def own_kernel(tiles, who, slot_table, recv, table, first, second, out, hit_out):
    shards = recv.shape[0]
    groups = out.shape[0]
    blocks = slot_table.shape[0]
    sub = subs()
    meta = meta_row(who[1])
    total = jnp.zeros((blocks, LANE), f32)
    hits = jnp.zeros((blocks, LANE), f32)
    slot = iota((blocks, LANE), 0) + 1
    for s in range(0, shards, 2):
        tile = recv[s, groups + tiles - 1].astype(f32) + recv[s + 1, groups + tiles - 1].astype(f32)
        place = jnp.sum(jnp.where(sub == meta, tile, 0.0), axis=0, keepdims=True)
        match = (slot == place.astype(jnp.int32)).astype(f32)
        rows = recv[s : s + 2, 0:groups].astype(f32).reshape(LANE, LANE).astype(bf16)
        total += dot(match.astype(bf16), rows, 1, 0)
        hits += match
    hits = dot(hits.astype(bf16), jnp.ones((LANE, LANE), bf16), 1, 0)
    hit_out[...] = hits
    sent = total.reshape(blocks // SUB, SUB, LANE).astype(bf16)
    column = pl.ds(who[0], blocks, stride=groups)
    weight = table[column, :]
    update, unused, unused_too = lamb_step(
        weight, first[column, :], second[column, :], sent.astype(f32).reshape(blocks, LANE)
    )
    update = jnp.where(hits > 0.5, update, 0.0)
    hot = table_hot(slot_table)
    sums = []
    for v in (weight, update):
        row = jnp.sum(v * v, axis=1, keepdims=True)
        sums.append(jnp.sum(jnp.where(hot, row, 0.0), axis=0, keepdims=True))
    both = split_rows(sums)
    dense = recv[0, groups:].astype(f32)
    for s in range(1, shards):
        dense = dense + recv[s, groups:].astype(f32)
    dense = dense.astype(bf16)
    for g in range(groups):
        out[g, 0 : blocks // SUB] = sent
        out[g, blocks // SUB : blocks // SUB + tiles] = dense
        out[g, blocks // SUB + tiles] = both


def owned(who, slot_table, recv, table, first, second, groups, tiles):
    blocks = slot_table.shape[0]
    return pl.pallas_call(
        functools.partial(own_kernel, tiles),
        out_shape=(
            jax.ShapeDtypeStruct((groups, blocks // SUB + tiles + 1, SUB, LANE), bf16),
            jax.ShapeDtypeStruct((blocks, LANE), f32),
        ),
        in_specs=[SMEM] + [VMEM] * 5,
        out_specs=(VMEM,) * 2,
        compiler_params=LIMIT,
        name="own",
    )(who, slot_table, recv, table, first, second)


def pack_kernel(tiles, recv, out):
    groups = recv.shape[0]
    start = recv.shape[1] - tiles - 1
    lines = recv[0, start:].astype(f32)
    for g in range(1, groups):
        lines = lines + recv[g, start:].astype(f32)
    dense = lines[0:tiles].astype(bf16)
    both = lines[tiles]
    both = split_rows((both[0:1] + both[1:2], both[2:3] + both[3:4]))
    for s in range(out.shape[0]):
        out[s, 0:tiles] = dense
        out[s, tiles] = both


def packed(recv, shards, tiles):
    return pl.pallas_call(
        functools.partial(pack_kernel, tiles),
        out_shape=jax.ShapeDtypeStruct((shards, tiles + 1, SUB, LANE), bf16),
        in_specs=[VMEM],
        out_specs=VMEM,
        compiler_params=LIMIT,
        name="pack",
    )(recv)


def slots_kernel(recv, hit, table, first, second, new_first, new_second, update_out):
    groups = recv.shape[0]
    blocks = hit.shape[0]
    touched = hit[...] > 0.5
    for g in range(groups):
        column = pl.ds(g, blocks, stride=groups)
        grad = recv[g, 0 : blocks // SUB].astype(f32).reshape(blocks, LANE)
        old_first, old_second = first[column, :], second[column, :]
        update, first_out, second_out = lamb_step(table[column, :], old_first, old_second, grad)
        new_first[column, :] = jnp.where(touched, first_out, old_first)
        new_second[column, :] = jnp.where(touched, second_out, old_second)
        update_out[column, :] = jnp.where(touched, update, 0.0)


def slots(recv, hit, table, first, second):
    shape = jax.ShapeDtypeStruct(table.shape, f32)
    return pl.pallas_call(
        slots_kernel,
        out_shape=(shape,) * 3,
        in_specs=[VMEM] * 5,
        out_specs=(VMEM,) * 3,
        cost_estimate=pl.CostEstimate(
            flops=2000 * table.size, bytes_accessed=24 * table.size, transcendentals=table.size
        ),
        compiler_params=LIMIT,
        name="slots",
    )(recv, hit, table, first, second)


def lamb_whole(weight, first_in, second_in, gradient):
    update, first_out, second_out = lamb_step(weight, first_in, second_in, gradient)
    ratio = jnp.sqrt(jnp.sum(weight * weight, keepdims=True)) / (
        jnp.sqrt(jnp.sum(update * update, keepdims=True)) + ratio_eps
    )
    return (weight - learn_rate * ratio * update, first_out, second_out)


def last_kernel(
    slot_table,
    recv,
    table,
    update,
    w_one,
    w_two,
    w_three,
    first_one,
    first_two,
    first_three,
    second_one,
    second_two,
    second_three,
    new_table,
    new_w_one,
    new_w_two,
    new_w_three,
    new_first_one,
    new_first_two,
    new_first_three,
    new_second_one,
    new_second_two,
    new_second_three,
    g_one,
    g_two,
    g_three,
):
    shards = recv.shape[0]
    tiles = recv.shape[1] - 1
    both = recv[0, tiles].astype(f32)
    for s in range(1, shards):
        both = both + recv[s, tiles].astype(f32)
    weight_sq = both[0:1] + both[1:2]
    update_sq = both[2:3] + both[3:4]
    ratio = learn_rate * (jnp.sqrt(weight_sq) / (jnp.sqrt(update_sq) + ratio_eps))
    ratio = jnp.sum(jnp.where(table_hot(slot_table), ratio, 0.0), axis=1, keepdims=True)
    blocks = slot_table.shape[0]
    groups = table.shape[0] // blocks
    for g in range(groups):
        column = pl.ds(g, blocks, stride=groups)
        new_table[column, :] = table[column, :] - ratio * update[column, :]
    pair = subs() // 2
    rows_two = g_two.shape[0] // shards
    rows_three = g_three.shape[0] // shards
    halves = g_two.shape[1] // LANE
    for s in range(shards):
        at = 0
        for h in range(halves):
            for r in range(0, rows_two, SUB):
                g_two[s * rows_two + r : s * rows_two + r + SUB, h * LANE : (h + 1) * LANE] = recv[
                    s, at
                ].astype(f32)
                at += 1
        for r in range(0, rows_three, SUB):
            g_three[s * rows_three + r : s * rows_three + r + SUB, :] = recv[s, at].astype(f32)
            at += 1
    for k in range(shards // 4):
        tile = jnp.zeros((SUB, LANE), f32)
        for a in range(4):
            tile = jnp.where(pair == a, recv[4 * k + a, tiles - 1].astype(f32), tile)
        c, r = k // 2, k % 2
        g_one[r * SUB : (r + 1) * SUB, c * LANE : (c + 1) * LANE] = tile
    for w, f, v, g, nw, nf, nv in (
        (w_one, first_one, second_one, g_one, new_w_one, new_first_one, new_second_one),
        (w_two, first_two, second_two, g_two, new_w_two, new_first_two, new_second_two),
        (w_three, first_three, second_three, g_three, new_w_three, new_first_three, new_second_three),
    ):
        nw[...], nf[...], nv[...] = lamb_whole(w[...], f[...], v[...], g[0 : w.shape[0], :])


def last(slot_table, recv, table, update, weights):
    outs = (table,) + weights
    return pl.pallas_call(
        last_kernel,
        out_shape=tuple(jax.ShapeDtypeStruct(a.shape, f32) for a in outs),
        in_specs=[VMEM] * 13,
        out_specs=(VMEM,) * 10,
        scratch_shapes=[
            pltpu.VMEM((2 * SUB, weights[0].shape[1]), f32),
            pltpu.VMEM(weights[1].shape, f32),
            pltpu.VMEM(weights[2].shape, f32),
        ],
        compiler_params=LIMIT,
        name="last",
    )(slot_table, recv, table, update, *weights)


def exchange(value, axis):
    return lax.all_to_all(value, axis, split_axis=0, concat_axis=0, tiled=True)


def body(
    table,
    table_first,
    table_second,
    slot_table,
    touched,
    emb_grads,
    block_slot,
    dense_x,
    dense_cot,
    w_one,
    w_two,
    w_three,
    first_one,
    first_two,
    first_three,
    second_one,
    second_two,
    second_three,
):
    shards = lax.axis_size(SHARD)
    groups = lax.axis_size("grp")
    blocks = table.shape[0]
    tiles = (w_two.size + w_three.size) // (shards * SUB * LANE) + 1
    who = jnp.stack([lax.axis_index("grp"), lax.axis_index(SHARD), lax.axis_index(SHARD[2])])
    who = who.astype(jnp.int32)
    flat = lambda a: a.reshape(-1, LANE)
    slot_column = slot_table[:, None]

    recv = exchange(
        routed(touched, flat(block_slot), flat(emb_grads), shards, blocks, groups), "grp"
    )
    dense = tower(dense_x, dense_cot, w_one, w_two, w_three, shards, tiles)
    recv = exchange(bucketed(who, recv, dense), SHARD)
    rows = flat(table), flat(table_first), flat(table_second)
    mine, hit = owned(who, slot_column, recv, *rows, groups, tiles)
    whole = exchange(mine, "grp")
    spread = exchange(packed(whole, shards, tiles), SHARD)
    new_first, new_second, update = slots(whole, hit, *rows)
    weights = (
        w_one,
        w_two,
        w_three,
        first_one,
        first_two,
        first_three,
        second_one,
        second_two,
        second_three,
    )
    new_table, *rest = last(slot_column, spread, rows[0], update, weights)
    back = [a.reshape(table.shape) for a in (new_table, new_first, new_second)]
    return (*back, *rest)


def solution(mesh):
    finer = Mesh(
        mesh.devices.reshape(mesh.shape["grp"], 4, 4, 2), ("grp", "shard_0", "shard_1", "shard_2")
    )
    rows = P(SHARD, None, None)
    placed = (
        rows,
        rows,
        rows,
        P(SHARD),
        P("grp", SHARD),
        P("grp", SHARD, None, None),
        P(),
        P(None, GRP_SHARD),
        P(GRP_SHARD, None),
    ) + (P(),) * 9
    return jax.shard_map(
        body,
        mesh=finer,
        in_specs=placed,
        out_specs=(rows, rows, rows) + (P(),) * 9,
        check_vma=False,
    )
```

```python
import functools
import jax
import jax.numpy as jnp
from jax import lax
from jax.experimental import pallas as pl
from jax.experimental.pallas import tpu as pltpu
from jax.sharding import Mesh
from jax.sharding import PartitionSpec as P

TABLES = 26
CAP = 8
SHARD = ("shard_0", "shard_1", "shard_2")
GRP_SHARD = ("grp", "shard_0", "shard_1", "shard_2")
SUB = 8
LANE = 128

beta_one = 0.9
beta_two = 0.999
corr_first = 1.0 - 0.9**10
corr_second = 1.0 - 0.999**10
adam_eps = 1e-06
decay_rate = 0.01
learn_rate = 0.1
ratio_eps = 1e-06

f32 = jnp.float32
bf16 = jnp.bfloat16
VMEM = pl.BlockSpec(memory_space=pltpu.VMEM)
SMEM = pl.BlockSpec(memory_space=pltpu.SMEM)
HBM = pl.BlockSpec(memory_space=pltpu.HBM)


LIMIT = pltpu.CompilerParams(vmem_limit_bytes=20 * 2**20)
WIDE = pltpu.CompilerParams(vmem_limit_bytes=53000 * 2**10)


def iota(shape, dim):
    return lax.broadcasted_iota(jnp.int32, shape, dim)


def subs():
    return iota((SUB, LANE), 0)


def dot(a, b, ca, cb):
    return lax.dot_general(a, b, (((ca,), (cb,)), ((), ())), preferred_element_type=f32)


def log_two(n):
    return n.bit_length() - 1


def route_kernel(shards, blocks, groups, ids, block_slot, grads, out, wide):
    count = ids.shape[1]
    wide[...] = grads[...].astype(f32)
    for g in range(groups):
        rows = wide[pl.ds(g, count, stride=groups), :]
        out[g, 0 : count // SUB] = rows.reshape(count // SUB, SUB, LANE).astype(bf16)
    table_rows = block_slot.shape[0]
    high = ids[...] >> log_two(LANE)
    low = ids[...] & (LANE - 1)
    high_hot = iota((table_rows, count), 0) == high
    low_hot = iota((LANE, count), 0) == low
    slot = block_slot[...]
    one = high_hot.astype(f32).astype(bf16)
    owner_of = (slot >> log_two(blocks)).astype(f32).astype(bf16)
    local_of = (slot & (blocks - 1)).astype(f32).astype(bf16)
    owner = jnp.sum(jnp.where(low_hot, dot(owner_of, one, 0, 0), 0.0), axis=0, keepdims=True)
    local = jnp.sum(jnp.where(low_hot, dot(local_of, one, 0, 0), 0.0), axis=0, keepdims=True)
    owner_hot = iota((shards, count), 0).astype(f32) == owner
    before = (iota((count, count), 0) < iota((count, count), 1)).astype(f32).astype(bf16)
    rank = dot(owner_hot.astype(f32).astype(bf16), before, 1, 0)
    rank = jnp.sum(jnp.where(owner_hot, rank, 0.0), axis=0, keepdims=True)
    sub = iota((SUB, count), 0)
    tile = jnp.where(sub == 0, owner * CAP + rank, jnp.where(sub == 1, local + 1.0, 0.0))
    tile = tile.astype(bf16)
    for g in range(groups):
        out[g, count // SUB] = tile


def routed(ids, block_slot, grads, shards, blocks, groups):
    count = ids.shape[1]
    return pl.pallas_call(
        functools.partial(route_kernel, shards, blocks, groups),
        out_shape=jax.ShapeDtypeStruct((groups, count // SUB + 1, SUB, LANE), bf16),
        in_specs=[VMEM] * 3,
        out_specs=VMEM,
        scratch_shapes=[pltpu.VMEM(grads.shape, f32)],
        name="route",
    )(ids, block_slot, grads)


def bucket_kernel(shards, who, recv, dense, out):
    groups = recv.shape[0]
    tiles = dense.shape[1]
    count = LANE
    local_rows = jnp.zeros((shards, LANE), f32)
    for g in range(groups):
        tile = recv[g, count // SUB].astype(f32)
        place = tile[0:1].astype(jnp.int32)
        picker = (iota((shards * CAP, count), 0) == place).astype(f32).astype(bf16)
        rows = recv[g, 0 : count // SUB].astype(f32).reshape(count, LANE).astype(bf16)
        out[:, g] = dot(picker, rows, 1, 0).reshape(shards, SUB, LANE).astype(bf16)
        owner = place >> log_two(CAP)
        lane = (place & (CAP - 1)) + g * CAP + who[2] * (LANE // 2)
        local = jnp.where(iota((shards, count), 0) == owner, tile[1:2], 0.0).astype(bf16)
        spot = (iota((LANE, count), 0) == lane).astype(f32).astype(bf16)
        local_rows += dot(local, spot, 1, 1)
    sub = subs()
    for s in range(shards):
        out[s, groups : groups + tiles - 1] = dense[s, 0 : tiles - 1]
        tile = dense[s, tiles - 1].astype(f32)
        tile = jnp.where(sub == meta_row(s), local_rows[s : s + 1], tile)
        out[s, groups + tiles - 1] = tile.astype(bf16)


def meta_row(s):
    return (2 * (s % 4) + 2) % SUB


def bucketed(who, recv, dense):
    shards, tiles = dense.shape[:2]
    return pl.pallas_call(
        functools.partial(bucket_kernel, shards),
        out_shape=jax.ShapeDtypeStruct((shards, recv.shape[0] + tiles, SUB, LANE), bf16),
        in_specs=[SMEM, VMEM, VMEM],
        out_specs=VMEM,
        compiler_params=LIMIT,
        name="bucket",
    )(who, recv, dense)


def act(half):
    bend = jnp.tanh(half)
    product = half * bend
    return (product + half).astype(bf16), (1.0 + bend) + (half - product * bend)


def tower_kernel(
    shards,
    parts,
    x_in,
    cot_in,
    w_one_in,
    w_two_in,
    w_three_in,
    out,
    x,
    cot,
    raw_one,
    raw_two,
    raw_three,
    w_one,
    w_two,
    w_two_t,
    w_three,
    g_one,
    g_two,
    g_three,
    sem,
    cot_sem,
):
    step = x.shape[1] // parts
    copies = [
        pltpu.make_async_copy(a, b, sem.at[i])
        for i, (a, b) in enumerate(
            ((w_one_in, raw_one), (x_in, x), (w_two_in, raw_two), (w_three_in, raw_three))
        )
    ]
    chunks = [
        pltpu.make_async_copy(
            cot_in.at[pl.ds(k * step, step), :], cot.at[pl.ds(k * step, step), :], cot_sem.at[k]
        )
        for k in range(parts)
    ]
    for c in copies + chunks:
        c.start()
    copies[0].wait()
    w_one[...] = (0.5 * raw_one[...]).astype(bf16)
    copies[1].wait()
    copies[2].wait()
    w_two[...] = (0.5 * raw_two[...]).astype(bf16)
    w_two_t[...] = (0.5 * raw_two[...]).T.astype(bf16)
    copies[3].wait()
    w_three[...] = (0.5 * raw_three[...]).astype(bf16)
    sums = None
    for k in range(parts):
        xs = x[:, k * step : (k + 1) * step]
        hidden_one, slope_one = act(dot(w_one[...], xs, 0, 0))
        hidden_two, slope_two = act(dot(w_two_t[...], hidden_one, 1, 0))
        chunks[k].wait()
        cots = cot[k * step : (k + 1) * step, :]
        three = dot(hidden_two, cots, 1, 0)
        back_two = (dot(w_three[...], cots, 1, 1) * slope_two).astype(bf16)
        two = dot(hidden_one, back_two, 1, 1)
        back_one = (dot(w_two[...], back_two, 1, 0) * slope_one).astype(bf16)
        one = dot(xs, back_one, 1, 1)
        if k == 0:
            g_one[0 : x.shape[0], :] = one
            g_two[...] = two
            g_three[...] = three
        else:
            g_one[0 : x.shape[0], :] += one
            g_two[...] += two
            g_three[...] += three
    g_one[x.shape[0] :, :] = jnp.zeros((g_one.shape[0] - x.shape[0], g_one.shape[1]), f32)
    rows_two = g_two.shape[0] // shards
    rows_three = g_three.shape[0] // shards
    halves = g_two.shape[1] // LANE
    for s in range(shards):
        at = 0
        for h in range(halves):
            for r in range(0, rows_two, SUB):
                out[s, at] = g_two[
                    s * rows_two + r : s * rows_two + r + SUB, h * LANE : (h + 1) * LANE
                ].astype(bf16)
                at += 1
        for r in range(0, rows_three, SUB):
            out[s, at] = g_three[s * rows_three + r : s * rows_three + r + SUB, :].astype(bf16)
            at += 1
        c, r = s // 4 // 2, s // 4 % 2
        out[s, at] = g_one[r * SUB : (r + 1) * SUB, c * LANE : (c + 1) * LANE].astype(bf16)


def tower(x, cot, w_one, w_two, w_three, shards, tiles, parts=4):
    din, samples = x.shape
    h_one, h_two = w_two.shape
    width = w_three.shape[1]
    macs = samples * (2 * din * h_one + 3 * h_one * h_two + 2 * h_two * width)
    return pl.pallas_call(
        functools.partial(tower_kernel, shards, parts),
        out_shape=jax.ShapeDtypeStruct((shards, tiles, SUB, LANE), bf16),
        in_specs=[HBM] * 5,
        out_specs=VMEM,
        scratch_shapes=[
            pltpu.VMEM(x.shape, bf16),
            pltpu.VMEM(cot.shape, bf16),
            pltpu.VMEM(w_one.shape, f32),
            pltpu.VMEM(w_two.shape, f32),
            pltpu.VMEM(w_three.shape, f32),
            pltpu.VMEM(w_one.shape, bf16),
            pltpu.VMEM(w_two.shape, bf16),
            pltpu.VMEM((h_two, h_one), bf16),
            pltpu.VMEM(w_three.shape, bf16),
            pltpu.VMEM((2 * SUB, h_one), f32),
            pltpu.VMEM((h_one, h_two), f32),
            pltpu.VMEM((h_two, width), f32),
            pltpu.SemaphoreType.DMA((4,)),
            pltpu.SemaphoreType.DMA((parts,)),
        ],
        cost_estimate=pl.CostEstimate(
            flops=2 * macs, bytes_accessed=4 * samples * width, transcendentals=samples * h_one
        ),
        compiler_params=pltpu.CompilerParams(vmem_limit_bytes=54000 * 2**10),
        name="tower",
    )(x, cot, w_one, w_two, w_three)


def lamb_step(weight, first_in, second_in, gradient):
    first_out = beta_one * first_in + (1.0 - beta_one) * gradient
    second_out = beta_two * second_in + (1.0 - beta_two) * gradient * gradient
    update = (
        first_out / corr_first / (jnp.sqrt(second_out / corr_second) + adam_eps)
        + decay_rate * weight
    )
    return update, first_out, second_out


def split_rows(rows):
    tile = jnp.zeros((SUB, LANE), f32)
    sub = subs()
    for i, row in enumerate(rows):
        high = row.astype(bf16).astype(f32)
        tile = jnp.where(sub == 2 * i, high, tile)
        tile = jnp.where(sub == 2 * i + 1, row - high, tile)
    return tile.astype(bf16)


def table_hot(slot_table):
    return slot_table[...] == iota((slot_table.shape[0], LANE), 1)


def own_kernel(tiles, who, slot_table, recv, table, first, second, out, hit_out):
    shards = recv.shape[0]
    groups = out.shape[0]
    blocks = slot_table.shape[0]
    sub = subs()
    meta = meta_row(who[1])
    total = jnp.zeros((blocks, LANE), f32)
    hits = jnp.zeros((blocks, LANE), f32)
    slot = iota((blocks, LANE), 0) + 1
    for s in range(0, shards, 2):
        tile = recv[s, groups + tiles - 1].astype(f32) + recv[s + 1, groups + tiles - 1].astype(f32)
        place = jnp.sum(jnp.where(sub == meta, tile, 0.0), axis=0, keepdims=True)
        match = (slot == place.astype(jnp.int32)).astype(f32)
        rows = recv[s : s + 2, 0:groups].astype(f32).reshape(LANE, LANE).astype(bf16)
        total += dot(match.astype(bf16), rows, 1, 0)
        hits += match
    hits = dot(hits.astype(bf16), jnp.ones((LANE, LANE), bf16), 1, 0)
    hit_out[...] = hits
    sent = total.reshape(blocks // SUB, SUB, LANE).astype(bf16)
    column = pl.ds(who[0], blocks, stride=groups)
    weight = table[column, :]
    update, unused, unused_too = lamb_step(
        weight, first[column, :], second[column, :], sent.astype(f32).reshape(blocks, LANE)
    )
    update = jnp.where(hits > 0.5, update, 0.0)
    hot = table_hot(slot_table)
    sums = []
    for v in (weight, update):
        row = jnp.sum(v * v, axis=1, keepdims=True)
        sums.append(jnp.sum(jnp.where(hot, row, 0.0), axis=0, keepdims=True))
    both = split_rows(sums)
    dense = recv[0, groups:].astype(f32)
    for s in range(1, shards):
        dense = dense + recv[s, groups:].astype(f32)
    dense = dense.astype(bf16)
    for g in range(groups):
        out[g, 0 : blocks // SUB] = sent
        out[g, blocks // SUB : blocks // SUB + tiles] = dense
        out[g, blocks // SUB + tiles] = both


def owned(who, slot_table, recv, table, first, second, groups, tiles):
    blocks = slot_table.shape[0]
    return pl.pallas_call(
        functools.partial(own_kernel, tiles),
        out_shape=(
            jax.ShapeDtypeStruct((groups, blocks // SUB + tiles + 1, SUB, LANE), bf16),
            jax.ShapeDtypeStruct((blocks, LANE), f32),
        ),
        in_specs=[SMEM] + [VMEM] * 5,
        out_specs=(VMEM,) * 2,
        compiler_params=LIMIT,
        name="own",
    )(who, slot_table, recv, table, first, second)


def pack_kernel(tiles, recv, out):
    groups = recv.shape[0]
    start = recv.shape[1] - tiles - 1
    lines = recv[0, start:].astype(f32)
    for g in range(1, groups):
        lines = lines + recv[g, start:].astype(f32)
    dense = lines[0:tiles].astype(bf16)
    both = lines[tiles]
    both = split_rows((both[0:1] + both[1:2], both[2:3] + both[3:4]))
    for s in range(out.shape[0]):
        out[s, 0:tiles] = dense
        out[s, tiles] = both


def packed(recv, shards, tiles):
    return pl.pallas_call(
        functools.partial(pack_kernel, tiles),
        out_shape=jax.ShapeDtypeStruct((shards, tiles + 1, SUB, LANE), bf16),
        in_specs=[VMEM],
        out_specs=VMEM,
        compiler_params=LIMIT,
        name="pack",
    )(recv)


def slots_kernel(
    recv,
    hit,
    table_in,
    first_in,
    second_in,
    new_first_out,
    new_second_out,
    update_out,
    table,
    first,
    second,
    update,
    sem,
    out_sem,
):
    groups = recv.shape[0]
    blocks = hit.shape[0]
    copies = [
        pltpu.make_async_copy(a, b, sem.at[i])
        for i, (a, b) in enumerate(((table_in, table), (first_in, first), (second_in, second)))
    ]
    for c in copies:
        c.start()
    touched = hit[...] > 0.5
    for c in copies:
        c.wait()
    for g in range(groups):
        column = pl.ds(g, blocks, stride=groups)
        grad = recv[g, 0 : blocks // SUB].astype(f32).reshape(blocks, LANE)
        old_first, old_second = first[column, :], second[column, :]
        change, first_out, second_out = lamb_step(table[column, :], old_first, old_second, grad)
        first[column, :] = jnp.where(touched, first_out, old_first)
        second[column, :] = jnp.where(touched, second_out, old_second)
        update[column, :] = jnp.where(touched, change, 0.0)
    copies = [
        pltpu.make_async_copy(a, b, out_sem.at[i])
        for i, (a, b) in enumerate(
            ((update, update_out), (first, new_first_out), (second, new_second_out))
        )
    ]
    for c in copies:
        c.start()
    for c in copies:
        c.wait()


def slots(recv, hit, table, first, second):
    shape = jax.ShapeDtypeStruct(table.shape, f32)
    return pl.pallas_call(
        slots_kernel,
        out_shape=(shape,) * 3,
        in_specs=[VMEM] * 2 + [HBM] * 3,
        out_specs=(HBM,) * 3,
        scratch_shapes=[pltpu.VMEM(table.shape, f32)] * 4
        + [pltpu.SemaphoreType.DMA((3,)), pltpu.SemaphoreType.DMA((3,))],
        cost_estimate=pl.CostEstimate(
            flops=2000 * table.size, bytes_accessed=24 * table.size, transcendentals=table.size
        ),
        compiler_params=WIDE,
        name="slots",
    )(recv, hit, table, first, second)


def lamb_whole(weight, first_in, second_in, gradient):
    update, first_out, second_out = lamb_step(weight, first_in, second_in, gradient)
    ratio = jnp.sqrt(jnp.sum(weight * weight, keepdims=True)) / (
        jnp.sqrt(jnp.sum(update * update, keepdims=True)) + ratio_eps
    )
    return (weight - learn_rate * ratio * update, first_out, second_out)


def last_kernel(slot_table, recv, *refs):
    ins, outs, scratch = refs[:11], refs[11:21], refs[21:]
    held, made, (g_one, g_two, g_three, sem, out_sem) = scratch[:11], scratch[11:21], scratch[21:]
    arrive = [pltpu.make_async_copy(a, b, sem.at[i]) for i, (a, b) in enumerate(zip(ins, held))]
    leave = [pltpu.make_async_copy(a, b, out_sem.at[i]) for i, (a, b) in enumerate(zip(made, outs))]
    for i in (3, 6, 9, 0, 1, 4, 7, 10, 2, 5, 8):
        arrive[i].start()
    shards = recv.shape[0]
    tiles = recv.shape[1] - 1
    both = recv[0, tiles].astype(f32)
    for s in range(1, shards):
        both = both + recv[s, tiles].astype(f32)
    weight_sq = both[0:1] + both[1:2]
    update_sq = both[2:3] + both[3:4]
    ratio = learn_rate * (jnp.sqrt(weight_sq) / (jnp.sqrt(update_sq) + ratio_eps))
    ratio = jnp.sum(jnp.where(table_hot(slot_table), ratio, 0.0), axis=1, keepdims=True)
    blocks = slot_table.shape[0]
    groups = ins[0].shape[0] // blocks
    pair = subs() // 2
    rows_two = g_two.shape[0] // shards
    rows_three = g_three.shape[0] // shards
    halves = g_two.shape[1] // LANE
    for s in range(shards):
        at = 0
        for h in range(halves):
            for r in range(0, rows_two, SUB):
                g_two[s * rows_two + r : s * rows_two + r + SUB, h * LANE : (h + 1) * LANE] = recv[
                    s, at
                ].astype(f32)
                at += 1
        for r in range(0, rows_three, SUB):
            g_three[s * rows_three + r : s * rows_three + r + SUB, :] = recv[s, at].astype(f32)
            at += 1
    for k in range(shards // 4):
        tile = jnp.zeros((SUB, LANE), f32)
        for a in range(4):
            tile = jnp.where(pair == a, recv[4 * k + a, tiles - 1].astype(f32), tile)
        c, r = k // 2, k % 2
        g_one[r * SUB : (r + 1) * SUB, c * LANE : (c + 1) * LANE] = tile

    def dense(n, gradient):
        for i in (2 + n, 5 + n, 8 + n):
            arrive[i].wait()
        weight, first, second = held[2 + n], held[5 + n], held[8 + n]
        made[1 + n][...], made[4 + n][...], made[7 + n][...] = lamb_whole(
            weight[...], first[...], second[...], gradient[0 : weight.shape[0], :]
        )
        for i in (1 + n, 4 + n, 7 + n):
            leave[i].start()

    dense(1, g_two)
    arrive[0].wait()
    arrive[1].wait()
    table, update = held[:2]
    for g in range(groups):
        column = pl.ds(g, blocks, stride=groups)
        made[0][column, :] = table[column, :] - ratio * update[column, :]
    leave[0].start()
    dense(2, g_three)
    dense(0, g_one)
    for c in leave:
        c.wait()


def last(slot_table, recv, table, update, weights):
    ins = (table, update) + weights
    outs = (table,) + weights
    return pl.pallas_call(
        last_kernel,
        out_shape=tuple(jax.ShapeDtypeStruct(a.shape, f32) for a in outs),
        in_specs=[VMEM] * 2 + [HBM] * 11,
        out_specs=(HBM,) * 10,
        scratch_shapes=[pltpu.VMEM(a.shape, f32) for a in ins + outs]
        + [
            pltpu.VMEM((2 * SUB, weights[0].shape[1]), f32),
            pltpu.VMEM(weights[1].shape, f32),
            pltpu.VMEM(weights[2].shape, f32),
            pltpu.SemaphoreType.DMA((len(ins),)),
            pltpu.SemaphoreType.DMA((len(outs),)),
        ],
        compiler_params=WIDE,
        name="last",
    )(slot_table, recv, *ins)


def exchange(value, axis):
    return lax.all_to_all(value, axis, split_axis=0, concat_axis=0, tiled=True)


def body(
    table,
    table_first,
    table_second,
    slot_table,
    touched,
    emb_grads,
    block_slot,
    dense_x,
    dense_cot,
    w_one,
    w_two,
    w_three,
    first_one,
    first_two,
    first_three,
    second_one,
    second_two,
    second_three,
):
    shards = lax.axis_size(SHARD)
    groups = lax.axis_size("grp")
    blocks = table.shape[0]
    tiles = (w_two.size + w_three.size) // (shards * SUB * LANE) + 1
    who = jnp.stack([lax.axis_index("grp"), lax.axis_index(SHARD), lax.axis_index(SHARD[2])])
    who = who.astype(jnp.int32)
    flat = lambda a: a.reshape(-1, LANE)
    slot_column = slot_table[:, None]

    recv = exchange(
        routed(touched, flat(block_slot), flat(emb_grads), shards, blocks, groups), "grp"
    )
    dense = tower(dense_x, dense_cot, w_one, w_two, w_three, shards, tiles)
    recv = exchange(bucketed(who, recv, dense), SHARD)
    rows = flat(table), flat(table_first), flat(table_second)
    mine, hit = owned(who, slot_column, recv, *rows, groups, tiles)
    whole = exchange(mine, "grp")
    spread = exchange(packed(whole, shards, tiles), SHARD)
    new_first, new_second, update = slots(whole, hit, *rows)
    weights = (
        w_one,
        w_two,
        w_three,
        first_one,
        first_two,
        first_three,
        second_one,
        second_two,
        second_three,
    )
    new_table, *rest = last(slot_column, spread, rows[0], update, weights)
    back = [a.reshape(table.shape) for a in (new_table, new_first, new_second)]
    return (*back, *rest)


def solution(mesh):
    finer = Mesh(
        mesh.devices.reshape(mesh.shape["grp"], 4, 4, 2), ("grp", "shard_0", "shard_1", "shard_2")
    )
    rows = P(SHARD, None, None)
    placed = (
        rows,
        rows,
        rows,
        P(SHARD),
        P("grp", SHARD),
        P("grp", SHARD, None, None),
        P(),
        P(None, GRP_SHARD),
        P(GRP_SHARD, None),
    ) + (P(),) * 9
    return jax.shard_map(
        body,
        mesh=finer,
        in_specs=placed,
        out_specs=(rows, rows, rows) + (P(),) * 9,
        check_vma=False,
    )
```

```python
import functools
import jax
import jax.numpy as jnp
from jax import lax
from jax.experimental import pallas as pl
from jax.experimental.pallas import tpu as pltpu
from jax.sharding import Mesh
from jax.sharding import PartitionSpec as P

TABLES = 26
CAP = 8
SHARD = ("shard_0", "shard_1", "shard_2")
GRP_SHARD = ("grp", "shard_0", "shard_1", "shard_2")
SUB = 8
LANE = 128

beta_one = 0.9
beta_two = 0.999
corr_first = 1.0 - 0.9**10
corr_second = 1.0 - 0.999**10
adam_eps = 1e-06
decay_rate = 0.01
learn_rate = 0.1
ratio_eps = 1e-06

f32 = jnp.float32
bf16 = jnp.bfloat16
VMEM = pl.BlockSpec(memory_space=pltpu.VMEM)
SMEM = pl.BlockSpec(memory_space=pltpu.SMEM)
HBM = pl.BlockSpec(memory_space=pltpu.HBM)


LIMIT = pltpu.CompilerParams(vmem_limit_bytes=20 * 2**20)
WIDE = pltpu.CompilerParams(vmem_limit_bytes=53000 * 2**10)


def iota(shape, dim):
    return lax.broadcasted_iota(jnp.int32, shape, dim)


def subs():
    return iota((SUB, LANE), 0)


def dot(a, b, ca, cb):
    return lax.dot_general(a, b, (((ca,), (cb,)), ((), ())), preferred_element_type=f32)


def log_two(n):
    return n.bit_length() - 1


def route_kernel(shards, blocks, groups, ids, block_slot, grads, out, wide):
    count = ids.shape[1]
    wide[...] = grads[...].astype(f32)
    for g in range(groups):
        rows = wide[pl.ds(g, count, stride=groups), :]
        out[g, 0 : count // SUB] = rows.reshape(count // SUB, SUB, LANE).astype(bf16)
    table_rows = block_slot.shape[0]
    high = ids[...] >> log_two(LANE)
    low = ids[...] & (LANE - 1)
    high_hot = iota((table_rows, count), 0) == high
    low_hot = iota((LANE, count), 0) == low
    slot = block_slot[...]
    one = high_hot.astype(f32).astype(bf16)
    owner_of = (slot >> log_two(blocks)).astype(f32).astype(bf16)
    local_of = (slot & (blocks - 1)).astype(f32).astype(bf16)
    owner = jnp.sum(jnp.where(low_hot, dot(owner_of, one, 0, 0), 0.0), axis=0, keepdims=True)
    local = jnp.sum(jnp.where(low_hot, dot(local_of, one, 0, 0), 0.0), axis=0, keepdims=True)
    owner_hot = iota((shards, count), 0).astype(f32) == owner
    before = (iota((count, count), 0) < iota((count, count), 1)).astype(f32).astype(bf16)
    rank = dot(owner_hot.astype(f32).astype(bf16), before, 1, 0)
    rank = jnp.sum(jnp.where(owner_hot, rank, 0.0), axis=0, keepdims=True)
    sub = iota((SUB, count), 0)
    tile = jnp.where(sub == 0, owner * CAP + rank, jnp.where(sub == 1, local + 1.0, 0.0))
    tile = tile.astype(bf16)
    for g in range(groups):
        out[g, count // SUB] = tile


def routed(ids, block_slot, grads, shards, blocks, groups):
    count = ids.shape[1]
    return pl.pallas_call(
        functools.partial(route_kernel, shards, blocks, groups),
        out_shape=jax.ShapeDtypeStruct((groups, count // SUB + 1, SUB, LANE), bf16),
        in_specs=[VMEM] * 3,
        out_specs=VMEM,
        scratch_shapes=[pltpu.VMEM(grads.shape, f32)],
        name="route",
    )(ids, block_slot, grads)


def bucket_kernel(shards, who, recv, dense, out, rows_out, last_out, sem):
    groups = recv.shape[0]
    tiles = dense.shape[1]
    count = LANE
    copies = [
        pltpu.make_async_copy(
            dense.at[:, 0 : tiles - 1], out.at[:, groups : groups + tiles - 1], sem.at[groups]
        )
    ]
    copies[0].start()
    local_rows = jnp.zeros((shards, LANE), f32)
    for g in range(groups):
        tile = recv[g, count // SUB].astype(f32)
        place = tile[0:1].astype(jnp.int32)
        picker = (iota((shards * CAP, count), 0) == place).astype(f32).astype(bf16)
        rows = recv[g, 0 : count // SUB].astype(f32).reshape(count, LANE).astype(bf16)
        rows_out[:, g] = dot(picker, rows, 1, 0).reshape(shards, SUB, LANE).astype(bf16)
        copies.append(pltpu.make_async_copy(rows_out.at[:, g], out.at[:, g], sem.at[g]))
        copies[-1].start()
        owner = place >> log_two(CAP)
        lane = (place & (CAP - 1)) + g * CAP + who[2] * (LANE // 2)
        local = jnp.where(iota((shards, count), 0) == owner, tile[1:2], 0.0).astype(bf16)
        spot = (iota((LANE, count), 0) == lane).astype(f32).astype(bf16)
        local_rows += dot(local, spot, 1, 1)
    sub = subs()
    for s in range(shards):
        tile = dense[s, tiles - 1].astype(f32)
        tile = jnp.where(sub == meta_row(s), local_rows[s : s + 1], tile)
        last_out[s] = tile.astype(bf16)
    copies.append(
        pltpu.make_async_copy(last_out, out.at[:, groups + tiles - 1], sem.at[groups + 1])
    )
    copies[-1].start()
    for c in copies:
        c.wait()


def meta_row(s):
    return (2 * (s % 4) + 2) % SUB


def bucketed(who, recv, dense):
    shards, tiles = dense.shape[:2]
    groups = recv.shape[0]
    return pl.pallas_call(
        functools.partial(bucket_kernel, shards),
        out_shape=jax.ShapeDtypeStruct((shards, groups + tiles, SUB, LANE), bf16),
        in_specs=[SMEM, VMEM, VMEM],
        out_specs=HBM,
        scratch_shapes=[
            pltpu.VMEM((shards, groups, SUB, LANE), bf16),
            pltpu.VMEM((shards, SUB, LANE), bf16),
            pltpu.SemaphoreType.DMA((groups + 2,)),
        ],
        compiler_params=LIMIT,
        name="bucket",
    )(who, recv, dense)


def act(half):
    bend = jnp.tanh(half)
    product = half * bend
    return (product + half).astype(bf16), (1.0 + bend) + (half - product * bend)


def tower_kernel(
    shards,
    parts,
    x_in,
    cot_in,
    w_one_in,
    w_two_in,
    w_three_in,
    out,
    x,
    cot,
    raw_one,
    raw_two,
    raw_three,
    w_one,
    w_two,
    w_two_t,
    w_three,
    g_one,
    g_two,
    g_three,
    sem,
    cot_sem,
):
    step = x.shape[1] // parts
    copies = [
        pltpu.make_async_copy(a, b, sem.at[i])
        for i, (a, b) in enumerate(
            ((w_one_in, raw_one), (x_in, x), (w_two_in, raw_two), (w_three_in, raw_three))
        )
    ]
    chunks = [
        pltpu.make_async_copy(
            cot_in.at[pl.ds(k * step, step), :], cot.at[pl.ds(k * step, step), :], cot_sem.at[k]
        )
        for k in range(parts)
    ]
    for c in copies + chunks:
        c.start()
    copies[0].wait()
    w_one[...] = (0.5 * raw_one[...]).astype(bf16)
    copies[1].wait()
    copies[2].wait()
    w_two[...] = (0.5 * raw_two[...]).astype(bf16)
    w_two_t[...] = (0.5 * raw_two[...]).T.astype(bf16)
    copies[3].wait()
    w_three[...] = (0.5 * raw_three[...]).astype(bf16)
    sums = None
    for k in range(parts):
        xs = x[:, k * step : (k + 1) * step]
        hidden_one, slope_one = act(dot(w_one[...], xs, 0, 0))
        hidden_two, slope_two = act(dot(w_two_t[...], hidden_one, 1, 0))
        chunks[k].wait()
        cots = cot[k * step : (k + 1) * step, :]
        three = dot(hidden_two, cots, 1, 0)
        back_two = (dot(w_three[...], cots, 1, 1) * slope_two).astype(bf16)
        two = dot(hidden_one, back_two, 1, 1)
        back_one = (dot(w_two[...], back_two, 1, 0) * slope_one).astype(bf16)
        one = dot(xs, back_one, 1, 1)
        if k == 0:
            g_one[0 : x.shape[0], :] = one
            g_two[...] = two
            g_three[...] = three
        else:
            g_one[0 : x.shape[0], :] += one
            g_two[...] += two
            g_three[...] += three
    g_one[x.shape[0] :, :] = jnp.zeros((g_one.shape[0] - x.shape[0], g_one.shape[1]), f32)
    rows_two = g_two.shape[0] // shards
    rows_three = g_three.shape[0] // shards
    halves = g_two.shape[1] // LANE
    for s in range(shards):
        at = 0
        for h in range(halves):
            for r in range(0, rows_two, SUB):
                out[s, at] = g_two[
                    s * rows_two + r : s * rows_two + r + SUB, h * LANE : (h + 1) * LANE
                ].astype(bf16)
                at += 1
        for r in range(0, rows_three, SUB):
            out[s, at] = g_three[s * rows_three + r : s * rows_three + r + SUB, :].astype(bf16)
            at += 1
        c, r = s // 4 // 2, s // 4 % 2
        out[s, at] = g_one[r * SUB : (r + 1) * SUB, c * LANE : (c + 1) * LANE].astype(bf16)


def tower(x, cot, w_one, w_two, w_three, shards, tiles, parts=4):
    din, samples = x.shape
    h_one, h_two = w_two.shape
    width = w_three.shape[1]
    macs = samples * (2 * din * h_one + 3 * h_one * h_two + 2 * h_two * width)
    return pl.pallas_call(
        functools.partial(tower_kernel, shards, parts),
        out_shape=jax.ShapeDtypeStruct((shards, tiles, SUB, LANE), bf16),
        in_specs=[HBM] * 5,
        out_specs=VMEM,
        scratch_shapes=[
            pltpu.VMEM(x.shape, bf16),
            pltpu.VMEM(cot.shape, bf16),
            pltpu.VMEM(w_one.shape, f32),
            pltpu.VMEM(w_two.shape, f32),
            pltpu.VMEM(w_three.shape, f32),
            pltpu.VMEM(w_one.shape, bf16),
            pltpu.VMEM(w_two.shape, bf16),
            pltpu.VMEM((h_two, h_one), bf16),
            pltpu.VMEM(w_three.shape, bf16),
            pltpu.VMEM((2 * SUB, h_one), f32),
            pltpu.VMEM((h_one, h_two), f32),
            pltpu.VMEM((h_two, width), f32),
            pltpu.SemaphoreType.DMA((4,)),
            pltpu.SemaphoreType.DMA((parts,)),
        ],
        cost_estimate=pl.CostEstimate(
            flops=2 * macs, bytes_accessed=4 * samples * width, transcendentals=samples * h_one
        ),
        compiler_params=pltpu.CompilerParams(vmem_limit_bytes=54000 * 2**10),
        name="tower",
    )(x, cot, w_one, w_two, w_three)


def lamb_step(weight, first_in, second_in, gradient):
    first_out = beta_one * first_in + (1.0 - beta_one) * gradient
    second_out = beta_two * second_in + (1.0 - beta_two) * gradient * gradient
    update = (first_out * (1.0 / corr_first)) / (
        jnp.sqrt(second_out * (1.0 / corr_second)) + adam_eps
    ) + decay_rate * weight
    return update, first_out, second_out


def with_sums(tile, piece, rows):
    row = (subs() - 2 * (piece % 4) - 2) & (SUB - 1)
    for i, value in enumerate(rows):
        high = value.astype(bf16).astype(f32)
        tile = jnp.where(row == 2 * i, high, tile)
        tile = jnp.where(row == 2 * i + 1, value - high, tile)
    return tile


def sums_in(tile, piece):
    row = ((subs() - 2 * (piece % 4) - 2) & (SUB - 1)) // 2
    return [jnp.sum(jnp.where(row == i, tile, 0.0), axis=0, keepdims=True) for i in range(2)]


def table_hot(slot_table):
    return slot_table[...] == iota((slot_table.shape[0], LANE), 1)


def own_kernel(tiles, who, slot_table, recv, table, first, second, out, hit_out):
    shards = recv.shape[0]
    groups = out.shape[0]
    blocks = slot_table.shape[0]
    sub = subs()
    meta = meta_row(who[1])
    total = jnp.zeros((blocks, LANE), f32)
    hits = jnp.zeros((blocks, LANE), f32)
    slot = iota((blocks, LANE), 0) + 1
    for s in range(0, shards, 2):
        tile = recv[s, groups + tiles - 1].astype(f32) + recv[s + 1, groups + tiles - 1].astype(f32)
        place = jnp.sum(jnp.where(sub == meta, tile, 0.0), axis=0, keepdims=True)
        match = (slot == place.astype(jnp.int32)).astype(f32)
        rows = recv[s : s + 2, 0:groups].astype(f32).reshape(LANE, LANE).astype(bf16)
        total += dot(match.astype(bf16), rows, 1, 0)
        hits += match
    hits = dot(hits.astype(bf16), jnp.ones((LANE, LANE), bf16), 1, 0)
    hit_out[...] = hits
    sent = total.reshape(blocks // SUB, SUB, LANE).astype(bf16)
    column = pl.ds(who[0], blocks, stride=groups)
    weight = table[column, :]
    update, unused, unused_too = lamb_step(
        weight, first[column, :], second[column, :], sent.astype(f32).reshape(blocks, LANE)
    )
    update = jnp.where(hits > 0.5, update, 0.0)
    hot = table_hot(slot_table)
    sums = []
    for v in (weight, update):
        row = jnp.sum(v * v, axis=1, keepdims=True)
        sums.append(jnp.sum(jnp.where(hot, row, 0.0), axis=0, keepdims=True))
    dense = recv[0, groups:].astype(f32)
    for s in range(1, shards):
        dense = dense + recv[s, groups:].astype(f32)
    mixed = with_sums(dense[tiles - 1], who[1], sums).astype(bf16)
    dense = dense[: tiles - 1].astype(bf16)
    for g in range(groups):
        out[g, 0 : blocks // SUB] = sent
        out[g, blocks // SUB : blocks // SUB + tiles - 1] = dense
        out[g, blocks // SUB + tiles - 1] = mixed


def owned(who, slot_table, recv, table, first, second, groups, tiles):
    blocks = slot_table.shape[0]
    return pl.pallas_call(
        functools.partial(own_kernel, tiles),
        out_shape=(
            jax.ShapeDtypeStruct((groups, blocks // SUB + tiles, SUB, LANE), bf16),
            jax.ShapeDtypeStruct((blocks, LANE), f32),
        ),
        in_specs=[SMEM] + [VMEM] * 5,
        out_specs=(VMEM,) * 2,
        compiler_params=LIMIT,
        name="own",
    )(who, slot_table, recv, table, first, second)


def pack_kernel(tiles, who, recv, out):
    groups = recv.shape[0]
    start = recv.shape[1] - tiles
    lines = recv[0, start:].astype(f32)
    for g in range(1, groups):
        lines = lines + recv[g, start:].astype(f32)
    dense = lines[: tiles - 1].astype(bf16)
    mixed = lines[tiles - 1]
    mixed = with_sums(mixed, who[1], sums_in(mixed, who[1])).astype(bf16)
    for s in range(out.shape[0]):
        out[s, 0 : tiles - 1] = dense
        out[s, tiles - 1] = mixed


def packed(who, recv, shards, tiles):
    return pl.pallas_call(
        functools.partial(pack_kernel, tiles),
        out_shape=jax.ShapeDtypeStruct((shards, tiles, SUB, LANE), bf16),
        in_specs=[SMEM, VMEM],
        out_specs=VMEM,
        compiler_params=LIMIT,
        name="pack",
    )(who, recv)


def slots_kernel(
    recv,
    hit,
    table_in,
    first_in,
    second_in,
    new_first_out,
    new_second_out,
    update_out,
    table,
    first,
    second,
    update,
    sem,
    out_sem,
):
    groups = recv.shape[0]
    blocks = hit.shape[0]
    copies = [
        pltpu.make_async_copy(a, b, sem.at[i])
        for i, (a, b) in enumerate(((table_in, table), (first_in, first), (second_in, second)))
    ]
    for c in copies:
        c.start()
    touched = hit[...] > 0.5
    for c in copies:
        c.wait()
    for g in range(groups):
        column = pl.ds(g, blocks, stride=groups)
        grad = recv[g, 0 : blocks // SUB].astype(f32).reshape(blocks, LANE)
        old_first, old_second = first[column, :], second[column, :]
        change, first_out, second_out = lamb_step(table[column, :], old_first, old_second, grad)
        first[column, :] = jnp.where(touched, first_out, old_first)
        second[column, :] = jnp.where(touched, second_out, old_second)
        update[column, :] = jnp.where(touched, change, 0.0)
    copies = [
        pltpu.make_async_copy(a, b, out_sem.at[i])
        for i, (a, b) in enumerate(
            ((update, update_out), (first, new_first_out), (second, new_second_out))
        )
    ]
    for c in copies:
        c.start()
    for c in copies:
        c.wait()


def slots(recv, hit, table, first, second):
    shape = jax.ShapeDtypeStruct(table.shape, f32)
    return pl.pallas_call(
        slots_kernel,
        out_shape=(shape,) * 3,
        in_specs=[VMEM] * 2 + [HBM] * 3,
        out_specs=(HBM,) * 3,
        scratch_shapes=[pltpu.VMEM(table.shape, f32)] * 4
        + [pltpu.SemaphoreType.DMA((3,)), pltpu.SemaphoreType.DMA((3,))],
        cost_estimate=pl.CostEstimate(
            flops=2000 * table.size, bytes_accessed=24 * table.size, transcendentals=table.size
        ),
        compiler_params=WIDE,
        name="slots",
    )(recv, hit, table, first, second)


def lamb_whole(weight, first_in, second_in, gradient):
    update, first_out, second_out = lamb_step(weight, first_in, second_in, gradient)
    ratio = jnp.sqrt(jnp.sum(weight * weight, keepdims=True)) / (
        jnp.sqrt(jnp.sum(update * update, keepdims=True)) + ratio_eps
    )
    return (weight - learn_rate * ratio * update, first_out, second_out)


def last_kernel(slot_table, recv, *refs):
    ins, outs, scratch = refs[:11], refs[11:21], refs[21:]
    held, made, (g_one, g_two, g_three, sem, out_sem) = scratch[:11], scratch[11:21], scratch[21:]
    arrive = [pltpu.make_async_copy(a, b, sem.at[i]) for i, (a, b) in enumerate(zip(ins, held))]
    leave = [pltpu.make_async_copy(a, b, out_sem.at[i]) for i, (a, b) in enumerate(zip(made, outs))]
    for i in (0, 1, 3, 6, 9, 4, 7, 10, 2, 5, 8):
        arrive[i].start()
    shards, tiles = recv.shape[:2]
    pieces = [sum(recv[s, tiles - 1].astype(f32) for s in range(a, shards, 4)) for a in range(4)]
    pieces = [sums_in(p, a) for a, p in enumerate(pieces)]
    weight_sq = sum(p[0] for p in pieces)
    update_sq = sum(p[1] for p in pieces)
    ratio = learn_rate * (jnp.sqrt(weight_sq) / (jnp.sqrt(update_sq) + ratio_eps))
    ratio = jnp.sum(jnp.where(table_hot(slot_table), ratio, 0.0), axis=1, keepdims=True)
    blocks = slot_table.shape[0]
    groups = ins[0].shape[0] // blocks
    arrive[0].wait()
    arrive[1].wait()
    table, update = held[:2]
    for g in range(groups):
        column = pl.ds(g, blocks, stride=groups)
        made[0][column, :] = table[column, :] - ratio * update[column, :]
    leave[0].start()
    pair = subs() // 2
    rows_two = g_two.shape[0] // shards
    rows_three = g_three.shape[0] // shards
    halves = g_two.shape[1] // LANE
    for s in range(shards):
        at = 0
        for h in range(halves):
            for r in range(0, rows_two, SUB):
                g_two[s * rows_two + r : s * rows_two + r + SUB, h * LANE : (h + 1) * LANE] = recv[
                    s, at
                ].astype(f32)
                at += 1
        for r in range(0, rows_three, SUB):
            g_three[s * rows_three + r : s * rows_three + r + SUB, :] = recv[s, at].astype(f32)
            at += 1
    for k in range(shards // 4):
        tile = jnp.zeros((SUB, LANE), f32)
        for a in range(4):
            tile = jnp.where(pair == a, recv[4 * k + a, tiles - 1].astype(f32), tile)
        c, r = k // 2, k % 2
        g_one[r * SUB : (r + 1) * SUB, c * LANE : (c + 1) * LANE] = tile

    def dense(n, gradient):
        for i in (2 + n, 5 + n, 8 + n):
            arrive[i].wait()
        weight, first, second = held[2 + n], held[5 + n], held[8 + n]
        made[1 + n][...], made[4 + n][...], made[7 + n][...] = lamb_whole(
            weight[...], first[...], second[...], gradient[0 : weight.shape[0], :]
        )
        for i in (1 + n, 4 + n, 7 + n):
            leave[i].start()

    dense(1, g_two)
    dense(2, g_three)
    dense(0, g_one)
    for c in leave:
        c.wait()


def last(slot_table, recv, table, update, weights):
    ins = (table, update) + weights
    outs = (table,) + weights
    return pl.pallas_call(
        last_kernel,
        out_shape=tuple(jax.ShapeDtypeStruct(a.shape, f32) for a in outs),
        in_specs=[VMEM] * 2 + [HBM] * 11,
        out_specs=(HBM,) * 10,
        scratch_shapes=[pltpu.VMEM(a.shape, f32) for a in ins + outs]
        + [
            pltpu.VMEM((2 * SUB, weights[0].shape[1]), f32),
            pltpu.VMEM(weights[1].shape, f32),
            pltpu.VMEM(weights[2].shape, f32),
            pltpu.SemaphoreType.DMA((len(ins),)),
            pltpu.SemaphoreType.DMA((len(outs),)),
        ],
        compiler_params=WIDE,
        name="last",
    )(slot_table, recv, *ins)


def exchange(value, axis):
    return lax.all_to_all(value, axis, split_axis=0, concat_axis=0, tiled=True)


def body(
    table,
    table_first,
    table_second,
    slot_table,
    touched,
    emb_grads,
    block_slot,
    dense_x,
    dense_cot,
    w_one,
    w_two,
    w_three,
    first_one,
    first_two,
    first_three,
    second_one,
    second_two,
    second_three,
):
    shards = lax.axis_size(SHARD)
    groups = lax.axis_size("grp")
    blocks = table.shape[0]
    tiles = (w_two.size + w_three.size) // (shards * SUB * LANE) + 1
    who = jnp.stack([lax.axis_index("grp"), lax.axis_index(SHARD), lax.axis_index(SHARD[2])])
    who = who.astype(jnp.int32)
    flat = lambda a: a.reshape(-1, LANE)
    slot_column = slot_table[:, None]

    recv = exchange(
        routed(touched, flat(block_slot), flat(emb_grads), shards, blocks, groups), "grp"
    )
    dense = tower(dense_x, dense_cot, w_one, w_two, w_three, shards, tiles)
    recv = exchange(bucketed(who, recv, dense), SHARD)
    rows = flat(table), flat(table_first), flat(table_second)
    mine, hit = owned(who, slot_column, recv, *rows, groups, tiles)
    whole = exchange(mine, "grp")
    spread = exchange(packed(who, whole, shards, tiles), SHARD)
    new_first, new_second, update = slots(whole, hit, *rows)
    weights = (
        w_one,
        w_two,
        w_three,
        first_one,
        first_two,
        first_three,
        second_one,
        second_two,
        second_three,
    )
    new_table, *rest = last(slot_column, spread, rows[0], update, weights)
    back = [a.reshape(table.shape) for a in (new_table, new_first, new_second)]
    return (*back, *rest)


def solution(mesh):
    finer = Mesh(
        mesh.devices.reshape(mesh.shape["grp"], 4, 4, 2), ("grp", "shard_0", "shard_1", "shard_2")
    )
    rows = P(SHARD, None, None)
    placed = (
        rows,
        rows,
        rows,
        P(SHARD),
        P("grp", SHARD),
        P("grp", SHARD, None, None),
        P(),
        P(None, GRP_SHARD),
        P(GRP_SHARD, None),
    ) + (P(),) * 9
    return jax.shard_map(
        body,
        mesh=finer,
        in_specs=placed,
        out_specs=(rows, rows, rows) + (P(),) * 9,
        check_vma=False,
    )
```

```python
import functools
import jax
import jax.numpy as jnp
from jax import lax
from jax.experimental import pallas as pl
from jax.experimental.pallas import tpu as pltpu
from jax.sharding import Mesh
from jax.sharding import PartitionSpec as P

TABLES = 26
CAP = 8
SHARD = ("shard_0", "shard_1", "shard_2")
GRP_SHARD = ("grp", "shard_0", "shard_1", "shard_2")
SUB = 8
LANE = 128
META_ROW = 2

beta_one = 0.9
beta_two = 0.999
corr_first = 1.0 - 0.9**10
corr_second = 1.0 - 0.999**10
adam_eps = 1e-06
decay_rate = 0.01
learn_rate = 0.1
ratio_eps = 1e-06

f32 = jnp.float32
bf16 = jnp.bfloat16
VMEM = pl.BlockSpec(memory_space=pltpu.VMEM)
SMEM = pl.BlockSpec(memory_space=pltpu.SMEM)
HBM = pl.BlockSpec(memory_space=pltpu.HBM)


LIMIT = pltpu.CompilerParams(vmem_limit_bytes=20 * 2**20)
WIDE = pltpu.CompilerParams(vmem_limit_bytes=53000 * 2**10)


def iota(shape, dim):
    return lax.broadcasted_iota(jnp.int32, shape, dim)


def subs():
    return iota((SUB, LANE), 0)


def turned(tile, rows):
    return pltpu.roll(tile, rows % SUB, 0) if rows % SUB else tile


def dot(a, b, ca, cb):
    return lax.dot_general(a, b, (((ca,), (cb,)), ((), ())), preferred_element_type=f32)


def log_two(n):
    return n.bit_length() - 1


def route_kernel(shards, blocks, groups, ids, block_slot, grads, out, wide):
    count = ids.shape[1]
    wide[...] = grads[...].astype(f32)
    for g in range(groups):
        rows = wide[pl.ds(g, count, stride=groups), :]
        out[g, 0 : count // SUB] = rows.reshape(count // SUB, SUB, LANE).astype(bf16)
    table_rows = block_slot.shape[0]
    high = ids[...] >> log_two(LANE)
    low = ids[...] & (LANE - 1)
    high_hot = iota((table_rows, count), 0) == high
    low_hot = iota((LANE, count), 0) == low
    slot = block_slot[...]
    one = high_hot.astype(f32).astype(bf16)
    owner_of = (slot >> log_two(blocks)).astype(f32).astype(bf16)
    local_of = (slot & (blocks - 1)).astype(f32).astype(bf16)
    owner = jnp.sum(jnp.where(low_hot, dot(owner_of, one, 0, 0), 0.0), axis=0, keepdims=True)
    local = jnp.sum(jnp.where(low_hot, dot(local_of, one, 0, 0), 0.0), axis=0, keepdims=True)
    owner_hot = iota((shards, count), 0).astype(f32) == owner
    before = (iota((count, count), 0) < iota((count, count), 1)).astype(f32).astype(bf16)
    rank = dot(owner_hot.astype(f32).astype(bf16), before, 1, 0)
    rank = jnp.sum(jnp.where(owner_hot, rank, 0.0), axis=0, keepdims=True)
    sub = iota((SUB, count), 0)
    tile = jnp.where(sub == 0, owner * CAP + rank, jnp.where(sub == 1, local + 1.0, 0.0))
    tile = tile.astype(bf16)
    for g in range(groups):
        out[g, count // SUB] = tile


def routed(ids, block_slot, grads, shards, blocks, groups):
    count = ids.shape[1]
    return pl.pallas_call(
        functools.partial(route_kernel, shards, blocks, groups),
        out_shape=jax.ShapeDtypeStruct((groups, count // SUB + 1, SUB, LANE), bf16),
        in_specs=[VMEM] * 3,
        out_specs=VMEM,
        scratch_shapes=[pltpu.VMEM(grads.shape, f32)],
        name="route",
    )(ids, block_slot, grads)


def bucket_kernel(shards, offset, recv, dense, out, rows_out, last_out, sem):
    groups = recv.shape[0]
    tiles = dense.shape[1]
    count = LANE
    copies = [
        pltpu.make_async_copy(
            dense.at[:, 0 : tiles - 1], out.at[:, groups : groups + tiles - 1], sem.at[groups]
        )
    ]
    copies[0].start()
    local_rows = jnp.zeros((shards, LANE), f32)
    for g in range(groups):
        tile = recv[g, count // SUB].astype(f32)
        place = tile[0:1].astype(jnp.int32)
        picker = (iota((shards * CAP, count), 0) == place).astype(f32).astype(bf16)
        rows = recv[g, 0 : count // SUB].astype(f32).reshape(count, LANE).astype(bf16)
        rows_out[:, g] = dot(picker, rows, 1, 0).reshape(shards, SUB, LANE).astype(bf16)
        copies.append(pltpu.make_async_copy(rows_out.at[:, g], out.at[:, g], sem.at[g]))
        copies[-1].start()
        owner = place >> log_two(CAP)
        lane = (place & (CAP - 1)) + g * CAP + offset[...]
        local = jnp.where(iota((shards, count), 0) == owner, tile[1:2], 0.0).astype(bf16)
        spot = (iota((LANE, count), 0) == lane).astype(f32).astype(bf16)
        local_rows += dot(local, spot, 1, 1)
    sub = subs()
    for s in range(shards):
        tile = dense[s, tiles - 1].astype(f32)
        tile = jnp.where(sub == META_ROW, local_rows[s : s + 1], tile)
        last_out[s] = tile.astype(bf16)
    copies.append(
        pltpu.make_async_copy(last_out, out.at[:, groups + tiles - 1], sem.at[groups + 1])
    )
    copies[-1].start()
    for c in copies:
        c.wait()


def bucketed(offset, recv, dense):
    shards, tiles = dense.shape[:2]
    groups = recv.shape[0]
    return pl.pallas_call(
        functools.partial(bucket_kernel, shards),
        out_shape=jax.ShapeDtypeStruct((shards, groups + tiles, SUB, LANE), bf16),
        in_specs=[VMEM] * 3,
        out_specs=HBM,
        scratch_shapes=[
            pltpu.VMEM((shards, groups, SUB, LANE), bf16),
            pltpu.VMEM((shards, SUB, LANE), bf16),
            pltpu.SemaphoreType.DMA((groups + 2,)),
        ],
        compiler_params=LIMIT,
        name="bucket",
    )(offset, recv, dense)


def act(half):
    bend = jnp.tanh(half)
    product = half * bend
    return (product + half).astype(bf16), (1.0 + bend) + (half - product * bend)


def tower_kernel(
    shards,
    parts,
    x_in,
    cot_in,
    w_one_in,
    w_two_in,
    w_three_in,
    out,
    x,
    cot,
    raw_one,
    raw_two,
    raw_three,
    w_one,
    w_two,
    w_two_t,
    w_three,
    g_one,
    g_two,
    g_three,
    sem,
    cot_sem,
):
    step = x.shape[1] // parts
    copies = [
        pltpu.make_async_copy(a, b, sem.at[i])
        for i, (a, b) in enumerate(
            ((w_one_in, raw_one), (x_in, x), (w_two_in, raw_two), (w_three_in, raw_three))
        )
    ]
    chunks = [
        pltpu.make_async_copy(
            cot_in.at[pl.ds(k * step, step), :], cot.at[pl.ds(k * step, step), :], cot_sem.at[k]
        )
        for k in range(parts)
    ]
    for c in copies + chunks:
        c.start()
    copies[0].wait()
    w_one[...] = (0.5 * raw_one[...]).astype(bf16)
    copies[1].wait()
    copies[2].wait()
    w_two[...] = (0.5 * raw_two[...]).astype(bf16)
    w_two_t[...] = (0.5 * raw_two[...]).T.astype(bf16)
    copies[3].wait()
    w_three[...] = (0.5 * raw_three[...]).astype(bf16)
    sums = None
    for k in range(parts):
        xs = x[:, k * step : (k + 1) * step]
        hidden_one, slope_one = act(dot(w_one[...], xs, 0, 0))
        hidden_two, slope_two = act(dot(w_two_t[...], hidden_one, 1, 0))
        chunks[k].wait()
        cots = cot[k * step : (k + 1) * step, :]
        three = dot(hidden_two, cots, 1, 0)
        back_two = (dot(w_three[...], cots, 1, 1) * slope_two).astype(bf16)
        two = dot(hidden_one, back_two, 1, 1)
        back_one = (dot(w_two[...], back_two, 1, 0) * slope_one).astype(bf16)
        one = dot(xs, back_one, 1, 1)
        if k == 0:
            g_one[0 : x.shape[0], :] = one
            g_two[...] = two
            g_three[...] = three
        else:
            g_one[0 : x.shape[0], :] += one
            g_two[...] += two
            g_three[...] += three
    g_one[x.shape[0] :, :] = jnp.zeros((g_one.shape[0] - x.shape[0], g_one.shape[1]), f32)
    rows_two = g_two.shape[0] // shards
    rows_three = g_three.shape[0] // shards
    halves = g_two.shape[1] // LANE
    for s in range(shards):
        at = 0
        for h in range(halves):
            for r in range(0, rows_two, SUB):
                out[s, at] = g_two[
                    s * rows_two + r : s * rows_two + r + SUB, h * LANE : (h + 1) * LANE
                ].astype(bf16)
                at += 1
        for r in range(0, rows_three, SUB):
            out[s, at] = g_three[s * rows_three + r : s * rows_three + r + SUB, :].astype(bf16)
            at += 1
        c, r = s // 4 // 2, s // 4 % 2
        tile = g_one[r * SUB : (r + 1) * SUB, c * LANE : (c + 1) * LANE]
        out[s, at] = turned(tile, -2 * (s % 4)).astype(bf16)


def tower(x, cot, w_one, w_two, w_three, shards, tiles, parts=4):
    din, samples = x.shape
    h_one, h_two = w_two.shape
    width = w_three.shape[1]
    macs = samples * (2 * din * h_one + 3 * h_one * h_two + 2 * h_two * width)
    return pl.pallas_call(
        functools.partial(tower_kernel, shards, parts),
        out_shape=jax.ShapeDtypeStruct((shards, tiles, SUB, LANE), bf16),
        in_specs=[HBM] * 5,
        out_specs=VMEM,
        scratch_shapes=[
            pltpu.VMEM(x.shape, bf16),
            pltpu.VMEM(cot.shape, bf16),
            pltpu.VMEM(w_one.shape, f32),
            pltpu.VMEM(w_two.shape, f32),
            pltpu.VMEM(w_three.shape, f32),
            pltpu.VMEM(w_one.shape, bf16),
            pltpu.VMEM(w_two.shape, bf16),
            pltpu.VMEM((h_two, h_one), bf16),
            pltpu.VMEM(w_three.shape, bf16),
            pltpu.VMEM((2 * SUB, h_one), f32),
            pltpu.VMEM((h_one, h_two), f32),
            pltpu.VMEM((h_two, width), f32),
            pltpu.SemaphoreType.DMA((4,)),
            pltpu.SemaphoreType.DMA((parts,)),
        ],
        cost_estimate=pl.CostEstimate(
            flops=2 * macs, bytes_accessed=4 * samples * width, transcendentals=samples * h_one
        ),
        compiler_params=pltpu.CompilerParams(vmem_limit_bytes=54000 * 2**10),
        name="tower",
    )(x, cot, w_one, w_two, w_three)


def lamb_step(weight, first_in, second_in, gradient):
    first_out = beta_one * first_in + (1.0 - beta_one) * gradient
    second_out = beta_two * second_in + (1.0 - beta_two) * gradient * gradient
    update = (first_out * (1.0 / corr_first)) / (
        jnp.sqrt(second_out * (1.0 / corr_second)) + adam_eps
    ) + decay_rate * weight
    return update, first_out, second_out


def with_sums(tile, rows):
    sub = subs()
    for i, value in enumerate(rows):
        high = value.astype(bf16).astype(f32)
        tile = jnp.where(sub == 2 * i + 2, high, tile)
        tile = jnp.where(sub == 2 * i + 3, value - high, tile)
    return tile


def sums_in(tile):
    return [tile[i : i + 1] + tile[i + 1 : i + 2] for i in (2, 4)]


def table_hot(slot_table):
    return slot_table[...] == iota((slot_table.shape[0], LANE), 1)


def own_kernel(tiles, slot_table, recv, table, first, second, out, hit_out):
    shards = recv.shape[0]
    groups = out.shape[0]
    blocks = slot_table.shape[0]
    total = jnp.zeros((blocks, LANE), f32)
    hits = jnp.zeros((blocks, LANE), f32)
    slot = iota((blocks, LANE), 0) + 1
    for s in range(0, shards, 2):
        tile = recv[s, groups + tiles - 1].astype(f32) + recv[s + 1, groups + tiles - 1].astype(f32)
        place = tile[META_ROW : META_ROW + 1]
        match = (slot == place.astype(jnp.int32)).astype(f32)
        rows = recv[s : s + 2, 0:groups].astype(f32).reshape(LANE, LANE).astype(bf16)
        total += dot(match.astype(bf16), rows, 1, 0)
        hits += match
    hits = dot(hits.astype(bf16), jnp.ones((LANE, LANE), bf16), 1, 0)
    hit_out[...] = hits
    sent = total.reshape(blocks // SUB, SUB, LANE).astype(bf16)
    weight = table[...]
    update, unused, unused_too = lamb_step(
        weight, first[...], second[...], sent.astype(f32).reshape(blocks, LANE)
    )
    update = jnp.where(hits > 0.5, update, 0.0)
    hot = table_hot(slot_table)
    sums = []
    for v in (weight, update):
        row = jnp.sum(v * v, axis=1, keepdims=True)
        sums.append(jnp.sum(jnp.where(hot, row, 0.0), axis=0, keepdims=True))
    dense = recv[0, groups:].astype(f32)
    for s in range(1, shards):
        dense = dense + recv[s, groups:].astype(f32)
    mixed = with_sums(dense[tiles - 1], sums).astype(bf16)
    dense = dense[: tiles - 1].astype(bf16)
    for g in range(groups):
        out[g, 0 : blocks // SUB] = sent
        out[g, blocks // SUB : blocks // SUB + tiles - 1] = dense
        out[g, blocks // SUB + tiles - 1] = mixed


def owned(slot_table, recv, table, first, second, groups, tiles):
    blocks = slot_table.shape[0]
    return pl.pallas_call(
        functools.partial(own_kernel, tiles),
        out_shape=(
            jax.ShapeDtypeStruct((groups, blocks // SUB + tiles, SUB, LANE), bf16),
            jax.ShapeDtypeStruct((blocks, LANE), f32),
        ),
        in_specs=[VMEM] * 5,
        out_specs=(VMEM,) * 2,
        compiler_params=LIMIT,
        name="own",
    )(slot_table, recv, table, first, second)


def pack_kernel(tiles, recv, out):
    groups = recv.shape[0]
    start = recv.shape[1] - tiles
    lines = recv[0, start:].astype(f32)
    for g in range(1, groups):
        lines = lines + recv[g, start:].astype(f32)
    dense = lines[: tiles - 1].astype(bf16)
    mixed = lines[tiles - 1]
    mixed = with_sums(mixed, sums_in(mixed)).astype(bf16)
    for s in range(out.shape[0]):
        out[s, 0 : tiles - 1] = dense
        out[s, tiles - 1] = mixed


def packed(recv, shards, tiles):
    return pl.pallas_call(
        functools.partial(pack_kernel, tiles),
        out_shape=jax.ShapeDtypeStruct((shards, tiles, SUB, LANE), bf16),
        in_specs=[VMEM],
        out_specs=VMEM,
        compiler_params=LIMIT,
        name="pack",
    )(recv)


def slots_kernel(
    recv,
    hit,
    table_in,
    first_in,
    second_in,
    new_first_out,
    new_second_out,
    update_out,
    table,
    first,
    second,
    update,
    sem,
    out_sem,
):
    groups = recv.shape[0]
    blocks = hit.shape[0]
    copies = [
        pltpu.make_async_copy(a, b, sem.at[i])
        for i, (a, b) in enumerate(((table_in, table), (first_in, first), (second_in, second)))
    ]
    for c in copies:
        c.start()
    touched = hit[...] > 0.5
    for c in copies:
        c.wait()
    for g in range(groups):
        column = pl.ds(g, blocks, stride=groups)
        grad = recv[g, 0 : blocks // SUB].astype(f32).reshape(blocks, LANE)
        old_first, old_second = first[column, :], second[column, :]
        change, first_out, second_out = lamb_step(table[column, :], old_first, old_second, grad)
        first[column, :] = jnp.where(touched, first_out, old_first)
        second[column, :] = jnp.where(touched, second_out, old_second)
        update[column, :] = jnp.where(touched, change, 0.0)
    copies = [
        pltpu.make_async_copy(a, b, out_sem.at[i])
        for i, (a, b) in enumerate(
            ((update, update_out), (first, new_first_out), (second, new_second_out))
        )
    ]
    for c in copies:
        c.start()
    for c in copies:
        c.wait()


def slots(recv, hit, table, first, second):
    shape = jax.ShapeDtypeStruct(table.shape, f32)
    return pl.pallas_call(
        slots_kernel,
        out_shape=(shape,) * 3,
        in_specs=[VMEM] * 2 + [HBM] * 3,
        out_specs=(HBM,) * 3,
        scratch_shapes=[pltpu.VMEM(table.shape, f32)] * 4
        + [pltpu.SemaphoreType.DMA((3,)), pltpu.SemaphoreType.DMA((3,))],
        cost_estimate=pl.CostEstimate(
            flops=2000 * table.size, bytes_accessed=24 * table.size, transcendentals=table.size
        ),
        compiler_params=WIDE,
        name="slots",
    )(recv, hit, table, first, second)


def lamb_whole(weight, first_in, second_in, gradient):
    update, first_out, second_out = lamb_step(weight, first_in, second_in, gradient)
    ratio = jnp.sqrt(jnp.sum(weight * weight, keepdims=True)) / (
        jnp.sqrt(jnp.sum(update * update, keepdims=True)) + ratio_eps
    )
    return (weight - learn_rate * ratio * update, first_out, second_out)


def last_kernel(slot_table, recv, *refs):
    ins, outs, scratch = refs[:11], refs[11:21], refs[21:]
    held, made, (g_one, g_two, g_three, sem, out_sem) = scratch[:11], scratch[11:21], scratch[21:]
    arrive = [pltpu.make_async_copy(a, b, sem.at[i]) for i, (a, b) in enumerate(zip(ins, held))]
    leave = [pltpu.make_async_copy(a, b, out_sem.at[i]) for i, (a, b) in enumerate(zip(made, outs))]
    for i in (0, 1, 3, 6, 9, 4, 7, 10, 2, 5, 8):
        arrive[i].start()
    shards, tiles = recv.shape[:2]
    pieces = recv[0, tiles - 1].astype(f32)
    for s in range(1, shards):
        pieces = pieces + recv[s, tiles - 1].astype(f32)
    weight_sq, update_sq = sums_in(pieces)
    ratio = learn_rate * (jnp.sqrt(weight_sq) / (jnp.sqrt(update_sq) + ratio_eps))
    ratio = jnp.sum(jnp.where(table_hot(slot_table), ratio, 0.0), axis=1, keepdims=True)
    blocks = slot_table.shape[0]
    groups = ins[0].shape[0] // blocks
    arrive[0].wait()
    arrive[1].wait()
    table, update = held[:2]
    for g in range(groups):
        column = pl.ds(g, blocks, stride=groups)
        made[0][column, :] = table[column, :] - ratio * update[column, :]
    leave[0].start()
    pair = subs() // 2
    rows_two = g_two.shape[0] // shards
    rows_three = g_three.shape[0] // shards
    halves = g_two.shape[1] // LANE
    for s in range(shards):
        at = 0
        for h in range(halves):
            for r in range(0, rows_two, SUB):
                g_two[s * rows_two + r : s * rows_two + r + SUB, h * LANE : (h + 1) * LANE] = recv[
                    s, at
                ].astype(f32)
                at += 1
        for r in range(0, rows_three, SUB):
            g_three[s * rows_three + r : s * rows_three + r + SUB, :] = recv[s, at].astype(f32)
            at += 1
    for k in range(shards // 4):
        tile = jnp.zeros((SUB, LANE), f32)
        for a in range(4):
            piece = turned(recv[4 * k + a, tiles - 1].astype(f32), 2 * a)
            tile = jnp.where(pair == a, piece, tile)
        c, r = k // 2, k % 2
        g_one[r * SUB : (r + 1) * SUB, c * LANE : (c + 1) * LANE] = tile

    def dense(n, gradient):
        for i in (2 + n, 5 + n, 8 + n):
            arrive[i].wait()
        weight, first, second = held[2 + n], held[5 + n], held[8 + n]
        made[1 + n][...], made[4 + n][...], made[7 + n][...] = lamb_whole(
            weight[...], first[...], second[...], gradient[0 : weight.shape[0], :]
        )
        for i in (1 + n, 4 + n, 7 + n):
            leave[i].start()

    dense(1, g_two)
    dense(2, g_three)
    dense(0, g_one)
    for c in leave:
        c.wait()


def last(slot_table, recv, table, update, weights):
    ins = (table, update) + weights
    outs = (table,) + weights
    return pl.pallas_call(
        last_kernel,
        out_shape=tuple(jax.ShapeDtypeStruct(a.shape, f32) for a in outs),
        in_specs=[VMEM] * 2 + [HBM] * 11,
        out_specs=(HBM,) * 10,
        scratch_shapes=[pltpu.VMEM(a.shape, f32) for a in ins + outs]
        + [
            pltpu.VMEM((2 * SUB, weights[0].shape[1]), f32),
            pltpu.VMEM(weights[1].shape, f32),
            pltpu.VMEM(weights[2].shape, f32),
            pltpu.SemaphoreType.DMA((len(ins),)),
            pltpu.SemaphoreType.DMA((len(outs),)),
        ],
        compiler_params=WIDE,
        name="last",
    )(slot_table, recv, *ins)


def exchange(value, axis):
    return lax.all_to_all(value, axis, split_axis=0, concat_axis=0, tiled=True)


def body(
    table,
    table_first,
    table_second,
    slot_table,
    touched,
    emb_grads,
    block_slot,
    dense_x,
    dense_cot,
    w_one,
    w_two,
    w_three,
    first_one,
    first_two,
    first_three,
    second_one,
    second_two,
    second_three,
):
    shards = lax.axis_size(SHARD)
    groups = lax.axis_size("grp")
    blocks = table.shape[0]
    tiles = (w_two.size + w_three.size) // (shards * SUB * LANE) + 1
    group = lax.axis_index("grp")
    offset = jnp.full((1, LANE), lax.axis_index(SHARD[2]) * (LANE // 2), jnp.int32)
    column = lambda a: lax.dynamic_index_in_dim(a, group, 1, keepdims=False)
    flat = lambda a: a.reshape(-1, LANE)
    slot_column = slot_table[:, None]

    recv = exchange(
        routed(touched, flat(block_slot), flat(emb_grads), shards, blocks, groups), "grp"
    )
    dense = tower(dense_x, dense_cot, w_one, w_two, w_three, shards, tiles)
    recv = exchange(bucketed(offset, recv, dense), SHARD)
    rows = flat(table), flat(table_first), flat(table_second)
    columns = [column(a) for a in (table, table_first, table_second)]
    mine, hit = owned(slot_column, recv, *columns, groups, tiles)
    whole = exchange(mine, "grp")
    spread = exchange(packed(whole, shards, tiles), SHARD)
    new_first, new_second, update = slots(whole, hit, *rows)
    weights = (
        w_one,
        w_two,
        w_three,
        first_one,
        first_two,
        first_three,
        second_one,
        second_two,
        second_three,
    )
    new_table, *rest = last(slot_column, spread, rows[0], update, weights)
    back = [a.reshape(table.shape) for a in (new_table, new_first, new_second)]
    return (*back, *rest)


def solution(mesh):
    finer = Mesh(
        mesh.devices.reshape(mesh.shape["grp"], 4, 4, 2), ("grp", "shard_0", "shard_1", "shard_2")
    )
    rows = P(SHARD, None, None)
    placed = (
        rows,
        rows,
        rows,
        P(SHARD),
        P("grp", SHARD),
        P("grp", SHARD, None, None),
        P(),
        P(None, GRP_SHARD),
        P(GRP_SHARD, None),
    ) + (P(),) * 9
    return jax.shard_map(
        body,
        mesh=finer,
        in_specs=placed,
        out_specs=(rows, rows, rows) + (P(),) * 9,
        check_vma=False,
    )
```

```python
import functools
import jax
import jax.numpy as jnp
from jax import lax
from jax.experimental import pallas as pl
from jax.experimental.pallas import tpu as pltpu
from jax.sharding import Mesh
from jax.sharding import PartitionSpec as P

TABLES = 26
CAP = 8
SHARD = ("shard_0", "shard_1", "shard_2")
GRP_SHARD = ("grp", "shard_0", "shard_1", "shard_2")
SUB = 8
LANE = 128
META_ROW = 2

beta_one = 0.9
beta_two = 0.999
corr_first = 1.0 - 0.9**10
corr_second = 1.0 - 0.999**10
adam_eps = 1e-06
decay_rate = 0.01
learn_rate = 0.1
ratio_eps = 1e-06

f32 = jnp.float32
bf16 = jnp.bfloat16
VMEM = pl.BlockSpec(memory_space=pltpu.VMEM)
SMEM = pl.BlockSpec(memory_space=pltpu.SMEM)
HBM = pl.BlockSpec(memory_space=pltpu.HBM)


LIMIT = pltpu.CompilerParams(vmem_limit_bytes=20 * 2**20)
WIDE = pltpu.CompilerParams(vmem_limit_bytes=53000 * 2**10)


def iota(shape, dim):
    return lax.broadcasted_iota(jnp.int32, shape, dim)


def subs():
    return iota((SUB, LANE), 0)


def turned(tile, rows):
    return pltpu.roll(tile, rows % SUB, 0) if rows % SUB else tile


def dot(a, b, ca, cb):
    return lax.dot_general(a, b, (((ca,), (cb,)), ((), ())), preferred_element_type=f32)


def log_two(n):
    return n.bit_length() - 1


def route_kernel(shards, blocks, groups, ids, block_slot, grads_in, out_hbm, grads, wide, out, sem):
    count = ids.shape[1]
    arrive = pltpu.make_async_copy(grads_in, grads, sem.at[groups])
    arrive.start()
    table_rows = block_slot.shape[0]
    high = ids[...] >> log_two(LANE)
    low = ids[...] & (LANE - 1)
    high_hot = iota((table_rows, count), 0) == high
    low_hot = iota((LANE, count), 0) == low
    slot = block_slot[...]
    one = high_hot.astype(f32).astype(bf16)
    owner_of = (slot >> log_two(blocks)).astype(f32).astype(bf16)
    local_of = (slot & (blocks - 1)).astype(f32).astype(bf16)
    owner = jnp.sum(jnp.where(low_hot, dot(owner_of, one, 0, 0), 0.0), axis=0, keepdims=True)
    local = jnp.sum(jnp.where(low_hot, dot(local_of, one, 0, 0), 0.0), axis=0, keepdims=True)
    owner_hot = iota((shards, count), 0).astype(f32) == owner
    before = (iota((count, count), 0) < iota((count, count), 1)).astype(f32).astype(bf16)
    rank = dot(owner_hot.astype(f32).astype(bf16), before, 1, 0)
    rank = jnp.sum(jnp.where(owner_hot, rank, 0.0), axis=0, keepdims=True)
    sub = iota((SUB, count), 0)
    tile = jnp.where(sub == 0, owner * CAP + rank, jnp.where(sub == 1, local + 1.0, 0.0))
    tile = tile.astype(bf16)
    arrive.wait()
    wide[...] = grads[...].astype(f32)
    leave = []
    for g in range(groups):
        rows = wide[pl.ds(g, count, stride=groups), :]
        out[g, 0 : count // SUB] = rows.reshape(count // SUB, SUB, LANE).astype(bf16)
        out[g, count // SUB] = tile
        leave.append(pltpu.make_async_copy(out.at[g], out_hbm.at[g], sem.at[g]))
        leave[-1].start()
    for c in leave:
        c.wait()


def routed(ids, block_slot, grads, shards, blocks, groups):
    count = ids.shape[1]
    shape = (groups, count // SUB + 1, SUB, LANE)
    return pl.pallas_call(
        functools.partial(route_kernel, shards, blocks, groups),
        out_shape=jax.ShapeDtypeStruct(shape, bf16),
        in_specs=[VMEM, VMEM, HBM],
        out_specs=HBM,
        scratch_shapes=[
            pltpu.VMEM(grads.shape, bf16),
            pltpu.VMEM(grads.shape, f32),
            pltpu.VMEM(shape, bf16),
            pltpu.SemaphoreType.DMA((groups + 1,)),
        ],
        name="route",
    )(ids, block_slot, grads)


def bucket_kernel(shards, offset, recv, dense, out, rows_out, last_out, sem):
    groups = recv.shape[0]
    tiles = dense.shape[1]
    count = LANE
    copies = [
        pltpu.make_async_copy(
            dense.at[:, 0 : tiles - 1], out.at[:, groups : groups + tiles - 1], sem.at[groups]
        )
    ]
    copies[0].start()
    local_rows = jnp.zeros((shards, LANE), f32)
    for g in range(groups):
        tile = recv[g, count // SUB].astype(f32)
        place = tile[0:1].astype(jnp.int32)
        picker = (iota((shards * CAP, count), 0) == place).astype(f32).astype(bf16)
        rows = recv[g, 0 : count // SUB].astype(f32).reshape(count, LANE).astype(bf16)
        rows_out[:, g] = dot(picker, rows, 1, 0).reshape(shards, SUB, LANE).astype(bf16)
        copies.append(pltpu.make_async_copy(rows_out.at[:, g], out.at[:, g], sem.at[g]))
        copies[-1].start()
        owner = place >> log_two(CAP)
        lane = (place & (CAP - 1)) + g * CAP + offset[...]
        local = jnp.where(iota((shards, count), 0) == owner, tile[1:2], 0.0).astype(bf16)
        spot = (iota((LANE, count), 0) == lane).astype(f32).astype(bf16)
        local_rows += dot(local, spot, 1, 1)
    sub = subs()
    for s in range(shards):
        tile = dense[s, tiles - 1].astype(f32)
        tile = jnp.where(sub == META_ROW, local_rows[s : s + 1], tile)
        last_out[s] = tile.astype(bf16)
    copies.append(
        pltpu.make_async_copy(last_out, out.at[:, groups + tiles - 1], sem.at[groups + 1])
    )
    copies[-1].start()
    for c in copies:
        c.wait()


def bucketed(offset, recv, dense):
    shards, tiles = dense.shape[:2]
    groups = recv.shape[0]
    return pl.pallas_call(
        functools.partial(bucket_kernel, shards),
        out_shape=jax.ShapeDtypeStruct((shards, groups + tiles, SUB, LANE), bf16),
        in_specs=[VMEM] * 3,
        out_specs=HBM,
        scratch_shapes=[
            pltpu.VMEM((shards, groups, SUB, LANE), bf16),
            pltpu.VMEM((shards, SUB, LANE), bf16),
            pltpu.SemaphoreType.DMA((groups + 2,)),
        ],
        compiler_params=LIMIT,
        name="bucket",
    )(offset, recv, dense)


def act(half):
    bend = jnp.tanh(half)
    product = half * bend
    return (product + half).astype(bf16), (1.0 + bend) + (half - product * bend)


def tower_kernel(
    shards,
    parts,
    x_in,
    cot_in,
    w_one_in,
    w_two_in,
    w_three_in,
    out,
    x,
    cot,
    raw_one,
    raw_two,
    raw_three,
    w_one,
    w_two,
    w_two_t,
    w_three,
    g_one,
    g_two,
    g_three,
    sem,
    cot_sem,
):
    step = x.shape[1] // parts
    copies = [
        pltpu.make_async_copy(a, b, sem.at[i])
        for i, (a, b) in enumerate(
            ((w_one_in, raw_one), (x_in, x), (w_two_in, raw_two), (w_three_in, raw_three))
        )
    ]
    chunks = [
        pltpu.make_async_copy(
            cot_in.at[pl.ds(k * step, step), :], cot.at[pl.ds(k * step, step), :], cot_sem.at[k]
        )
        for k in range(parts)
    ]
    for c in copies + chunks:
        c.start()
    copies[0].wait()
    w_one[...] = (0.5 * raw_one[...]).astype(bf16)
    copies[1].wait()
    copies[2].wait()
    w_two[...] = (0.5 * raw_two[...]).astype(bf16)
    w_two_t[...] = (0.5 * raw_two[...]).T.astype(bf16)
    copies[3].wait()
    w_three[...] = (0.5 * raw_three[...]).astype(bf16)
    samples = lambda k: slice(k * step, (k + 1) * step)
    first, second = {}, {}

    def layer_one(k):
        first[k] = act(dot(w_one[...], x[:, samples(k)], 0, 0))

    def layer_two(k):
        hidden, slope = act(dot(w_two_t[...], first[k][0], 1, 0))
        chunks[k].wait()
        back = dot(w_three[...], cot[samples(k), :], 1, 1) * slope
        second[k] = hidden, back.astype(bf16)

    def add(k, total, value):
        total[...] = value if k == 0 else total[...] + value

    def gradients(k):
        hidden_one, slope_one = first.pop(k)
        hidden_two, back_two = second.pop(k)
        add(k, g_three, dot(hidden_two, cot[samples(k), :], 1, 0))
        add(k, g_two, dot(hidden_one, back_two, 1, 1))
        back_one = (dot(w_two[...], back_two, 1, 0) * slope_one).astype(bf16)
        add(k, g_one.at[0 : x.shape[0], :], dot(x[:, samples(k)], back_one, 1, 1))

    for k in range(parts + 2):
        if k < parts:
            layer_one(k)
        if k > 1:
            gradients(k - 2)
        if 0 < k <= parts:
            layer_two(k - 1)
    g_one[x.shape[0] :, :] = jnp.zeros((g_one.shape[0] - x.shape[0], g_one.shape[1]), f32)
    rows_two = g_two.shape[0] // shards
    rows_three = g_three.shape[0] // shards
    halves = g_two.shape[1] // LANE
    for s in range(shards):
        at = 0
        for h in range(halves):
            for r in range(0, rows_two, SUB):
                out[s, at] = g_two[
                    s * rows_two + r : s * rows_two + r + SUB, h * LANE : (h + 1) * LANE
                ].astype(bf16)
                at += 1
        for r in range(0, rows_three, SUB):
            out[s, at] = g_three[s * rows_three + r : s * rows_three + r + SUB, :].astype(bf16)
            at += 1
        c, r = s // 4 // 2, s // 4 % 2
        tile = g_one[r * SUB : (r + 1) * SUB, c * LANE : (c + 1) * LANE]
        out[s, at] = turned(tile, -2 * (s % 4)).astype(bf16)


def tower(x, cot, w_one, w_two, w_three, shards, tiles, parts=8):
    din, samples = x.shape
    h_one, h_two = w_two.shape
    width = w_three.shape[1]
    macs = samples * (2 * din * h_one + 3 * h_one * h_two + 2 * h_two * width)
    return pl.pallas_call(
        functools.partial(tower_kernel, shards, parts),
        out_shape=jax.ShapeDtypeStruct((shards, tiles, SUB, LANE), bf16),
        in_specs=[HBM] * 5,
        out_specs=VMEM,
        scratch_shapes=[
            pltpu.VMEM(x.shape, bf16),
            pltpu.VMEM(cot.shape, bf16),
            pltpu.VMEM(w_one.shape, f32),
            pltpu.VMEM(w_two.shape, f32),
            pltpu.VMEM(w_three.shape, f32),
            pltpu.VMEM(w_one.shape, bf16),
            pltpu.VMEM(w_two.shape, bf16),
            pltpu.VMEM((h_two, h_one), bf16),
            pltpu.VMEM(w_three.shape, bf16),
            pltpu.VMEM((2 * SUB, h_one), f32),
            pltpu.VMEM((h_one, h_two), f32),
            pltpu.VMEM((h_two, width), f32),
            pltpu.SemaphoreType.DMA((4,)),
            pltpu.SemaphoreType.DMA((parts,)),
        ],
        cost_estimate=pl.CostEstimate(
            flops=2 * macs, bytes_accessed=4 * samples * width, transcendentals=samples * h_one
        ),
        compiler_params=pltpu.CompilerParams(vmem_limit_bytes=54000 * 2**10),
        name="tower",
    )(x, cot, w_one, w_two, w_three)


def lamb_step(weight, first_in, second_in, gradient):
    first_out = beta_one * first_in + (1.0 - beta_one) * gradient
    second_out = beta_two * second_in + (1.0 - beta_two) * gradient * gradient
    update = (first_out * (1.0 / corr_first)) / (
        jnp.sqrt(second_out * (1.0 / corr_second)) + adam_eps
    ) + decay_rate * weight
    return update, first_out, second_out


def with_sums(tile, rows):
    sub = subs()
    for i, value in enumerate(rows):
        high = value.astype(bf16).astype(f32)
        tile = jnp.where(sub == 2 * i + 2, high, tile)
        tile = jnp.where(sub == 2 * i + 3, value - high, tile)
    return tile


def sums_in(tile):
    return [tile[i : i + 1] + tile[i + 1 : i + 2] for i in (2, 4)]


def table_hot(slot_table):
    return slot_table[...] == iota((slot_table.shape[0], LANE), 1)


def own_kernel(tiles, slot_table, recv, table, first, second, out, hit_out):
    shards = recv.shape[0]
    groups = out.shape[0]
    blocks = slot_table.shape[0]
    total = jnp.zeros((blocks, LANE), f32)
    hits = jnp.zeros((blocks, LANE), f32)
    slot = iota((blocks, LANE), 0) + 1
    for s in range(0, shards, 2):
        tile = recv[s, groups + tiles - 1].astype(f32) + recv[s + 1, groups + tiles - 1].astype(f32)
        place = tile[META_ROW : META_ROW + 1]
        match = (slot == place.astype(jnp.int32)).astype(f32)
        rows = recv[s : s + 2, 0:groups].astype(f32).reshape(LANE, LANE).astype(bf16)
        total += dot(match.astype(bf16), rows, 1, 0)
        hits += match
    hits = dot(hits.astype(bf16), jnp.ones((LANE, LANE), bf16), 1, 0)
    hit_out[...] = hits
    sent = total.reshape(blocks // SUB, SUB, LANE).astype(bf16)
    weight = table[...]
    update, unused, unused_too = lamb_step(
        weight, first[...], second[...], sent.astype(f32).reshape(blocks, LANE)
    )
    update = jnp.where(hits > 0.5, update, 0.0)
    hot = table_hot(slot_table)
    sums = []
    for v in (weight, update):
        row = jnp.sum(v * v, axis=1, keepdims=True)
        sums.append(jnp.sum(jnp.where(hot, row, 0.0), axis=0, keepdims=True))
    dense = recv[0, groups:].astype(f32)
    for s in range(1, shards):
        dense = dense + recv[s, groups:].astype(f32)
    mixed = with_sums(dense[tiles - 1], sums).astype(bf16)
    dense = dense[: tiles - 1].astype(bf16)
    for g in range(groups):
        out[g, 0 : blocks // SUB] = sent
        out[g, blocks // SUB : blocks // SUB + tiles - 1] = dense
        out[g, blocks // SUB + tiles - 1] = mixed


def owned(slot_table, recv, table, first, second, groups, tiles):
    blocks = slot_table.shape[0]
    return pl.pallas_call(
        functools.partial(own_kernel, tiles),
        out_shape=(
            jax.ShapeDtypeStruct((groups, blocks // SUB + tiles, SUB, LANE), bf16),
            jax.ShapeDtypeStruct((blocks, LANE), f32),
        ),
        in_specs=[VMEM] * 5,
        out_specs=(VMEM,) * 2,
        compiler_params=LIMIT,
        name="own",
    )(slot_table, recv, table, first, second)


def pack_kernel(tiles, recv, out):
    groups = recv.shape[0]
    start = recv.shape[1] - tiles
    lines = recv[0, start:].astype(f32)
    for g in range(1, groups):
        lines = lines + recv[g, start:].astype(f32)
    dense = lines[: tiles - 1].astype(bf16)
    mixed = lines[tiles - 1]
    mixed = with_sums(mixed, sums_in(mixed)).astype(bf16)
    for s in range(out.shape[0]):
        out[s, 0 : tiles - 1] = dense
        out[s, tiles - 1] = mixed


def packed(recv, shards, tiles):
    return pl.pallas_call(
        functools.partial(pack_kernel, tiles),
        out_shape=jax.ShapeDtypeStruct((shards, tiles, SUB, LANE), bf16),
        in_specs=[VMEM],
        out_specs=VMEM,
        compiler_params=LIMIT,
        name="pack",
    )(recv)


def slots_kernel(
    recv,
    hit,
    table_in,
    first_in,
    second_in,
    new_first_out,
    new_second_out,
    update,
    table,
    first,
    second,
    sem,
    out_sem,
):
    groups = recv.shape[0]
    blocks = hit.shape[0]
    copies = [
        pltpu.make_async_copy(a, b, sem.at[i])
        for i, (a, b) in enumerate(((table_in, table), (first_in, first), (second_in, second)))
    ]
    for c in copies:
        c.start()
    touched = hit[...] > 0.5
    for c in copies:
        c.wait()
    for g in range(groups):
        column = pl.ds(g, blocks, stride=groups)
        grad = recv[g, 0 : blocks // SUB].astype(f32).reshape(blocks, LANE)
        old_first, old_second = first[column, :], second[column, :]
        change, first_out, second_out = lamb_step(table[column, :], old_first, old_second, grad)
        first[column, :] = jnp.where(touched, first_out, old_first)
        second[column, :] = jnp.where(touched, second_out, old_second)
        update[column, :] = jnp.where(touched, change, 0.0)
    leave = [
        pltpu.make_async_copy(a, b, out_sem.at[i])
        for i, (a, b) in enumerate(((first, new_first_out), (second, new_second_out)))
    ]
    for c in leave:
        c.start()
    for c in leave:
        c.wait()


def slots(recv, hit, table, first, second):
    shape = jax.ShapeDtypeStruct(table.shape, f32)
    return pl.pallas_call(
        slots_kernel,
        out_shape=(shape,) * 3,
        in_specs=[VMEM] * 2 + [HBM] * 3,
        out_specs=(HBM,) * 2 + (VMEM,),
        scratch_shapes=[pltpu.VMEM(table.shape, f32)] * 3
        + [pltpu.SemaphoreType.DMA((3,)), pltpu.SemaphoreType.DMA((2,))],
        cost_estimate=pl.CostEstimate(
            flops=2000 * table.size, bytes_accessed=24 * table.size, transcendentals=table.size
        ),
        compiler_params=WIDE,
        name="slots",
    )(recv, hit, table, first, second)


def lamb_whole(weight, first_in, second_in, gradient):
    update, first_out, second_out = lamb_step(weight, first_in, second_in, gradient)
    ratio = jnp.sqrt(jnp.sum(weight * weight, keepdims=True)) / (
        jnp.sqrt(jnp.sum(update * update, keepdims=True)) + ratio_eps
    )
    return (weight - learn_rate * ratio * update, first_out, second_out)


def last_kernel(slot_table, recv, table, update, *refs):
    ins, outs, scratch = refs[:9], refs[9:19], refs[19:]
    held, made, (g_one, g_two, g_three, sem, out_sem) = scratch[:9], scratch[9:19], scratch[19:]
    arrive = [pltpu.make_async_copy(a, b, sem.at[i]) for i, (a, b) in enumerate(zip(ins, held))]
    leave = [pltpu.make_async_copy(a, b, out_sem.at[i]) for i, (a, b) in enumerate(zip(made, outs))]
    for i in (1, 4, 7, 2, 5, 8, 0, 3, 6):
        arrive[i].start()
    shards, tiles = recv.shape[:2]
    pieces = recv[0, tiles - 1].astype(f32)
    for s in range(1, shards):
        pieces = pieces + recv[s, tiles - 1].astype(f32)
    weight_sq, update_sq = sums_in(pieces)
    ratio = learn_rate * (jnp.sqrt(weight_sq) / (jnp.sqrt(update_sq) + ratio_eps))
    ratio = jnp.sum(jnp.where(table_hot(slot_table), ratio, 0.0), axis=1, keepdims=True)
    blocks = slot_table.shape[0]
    groups = table.shape[0] // blocks
    for g in range(groups):
        column = pl.ds(g, blocks, stride=groups)
        made[0][column, :] = table[column, :] - ratio * update[column, :]
    leave[0].start()
    pair = subs() // 2
    rows_two = g_two.shape[0] // shards
    rows_three = g_three.shape[0] // shards
    halves = g_two.shape[1] // LANE
    for s in range(shards):
        at = 0
        for h in range(halves):
            for r in range(0, rows_two, SUB):
                g_two[s * rows_two + r : s * rows_two + r + SUB, h * LANE : (h + 1) * LANE] = recv[
                    s, at
                ].astype(f32)
                at += 1
        for r in range(0, rows_three, SUB):
            g_three[s * rows_three + r : s * rows_three + r + SUB, :] = recv[s, at].astype(f32)
            at += 1
    for k in range(shards // 4):
        tile = jnp.zeros((SUB, LANE), f32)
        for a in range(4):
            piece = turned(recv[4 * k + a, tiles - 1].astype(f32), 2 * a)
            tile = jnp.where(pair == a, piece, tile)
        c, r = k // 2, k % 2
        g_one[r * SUB : (r + 1) * SUB, c * LANE : (c + 1) * LANE] = tile

    def dense(n, gradient):
        for i in (n, 3 + n, 6 + n):
            arrive[i].wait()
        weight, first, second = held[n], held[3 + n], held[6 + n]
        made[1 + n][...], made[4 + n][...], made[7 + n][...] = lamb_whole(
            weight[...], first[...], second[...], gradient[0 : weight.shape[0], :]
        )
        for i in (1 + n, 4 + n, 7 + n):
            leave[i].start()

    dense(1, g_two)
    dense(2, g_three)
    dense(0, g_one)
    for c in leave:
        c.wait()


def last(slot_table, recv, table, update, weights):
    outs = (table,) + weights
    return pl.pallas_call(
        last_kernel,
        out_shape=tuple(jax.ShapeDtypeStruct(a.shape, f32) for a in outs),
        in_specs=[VMEM] * 4 + [HBM] * 9,
        out_specs=(HBM,) * 10,
        scratch_shapes=[pltpu.VMEM(a.shape, f32) for a in weights + outs]
        + [
            pltpu.VMEM((2 * SUB, weights[0].shape[1]), f32),
            pltpu.VMEM(weights[1].shape, f32),
            pltpu.VMEM(weights[2].shape, f32),
            pltpu.SemaphoreType.DMA((len(weights),)),
            pltpu.SemaphoreType.DMA((len(outs),)),
        ],
        compiler_params=WIDE,
        name="last",
    )(slot_table, recv, table, update, *weights)


def exchange(value, axis):
    return lax.all_to_all(value, axis, split_axis=0, concat_axis=0, tiled=True)


def body(
    table,
    table_first,
    table_second,
    slot_table,
    touched,
    emb_grads,
    block_slot,
    dense_x,
    dense_cot,
    w_one,
    w_two,
    w_three,
    first_one,
    first_two,
    first_three,
    second_one,
    second_two,
    second_three,
):
    shards = lax.axis_size(SHARD)
    groups = lax.axis_size("grp")
    blocks = table.shape[0]
    tiles = (w_two.size + w_three.size) // (shards * SUB * LANE) + 1
    group = lax.axis_index("grp")
    offset = jnp.full((1, LANE), lax.axis_index(SHARD[2]) * (LANE // 2), jnp.int32)
    column = lambda a: lax.dynamic_index_in_dim(a, group, 1, keepdims=False)
    flat = lambda a: a.reshape(-1, LANE)
    slot_column = slot_table[:, None]

    recv = exchange(
        routed(touched, flat(block_slot), flat(emb_grads), shards, blocks, groups), "grp"
    )
    dense = tower(dense_x, dense_cot, w_one, w_two, w_three, shards, tiles)
    recv = exchange(bucketed(offset, recv, dense), SHARD)
    rows = flat(table), flat(table_first), flat(table_second)
    columns = [column(a) for a in (table, table_first, table_second)]
    mine, hit = owned(slot_column, recv, *columns, groups, tiles)
    whole = exchange(mine, "grp")
    spread = exchange(packed(whole, shards, tiles), SHARD)
    new_first, new_second, update = slots(whole, hit, *rows)
    weights = (
        w_one,
        w_two,
        w_three,
        first_one,
        first_two,
        first_three,
        second_one,
        second_two,
        second_three,
    )
    new_table, *rest = last(slot_column, spread, rows[0], update, weights)
    back = [a.reshape(table.shape) for a in (new_table, new_first, new_second)]
    return (*back, *rest)


def solution(mesh):
    finer = Mesh(
        mesh.devices.reshape(mesh.shape["grp"], 4, 4, 2), ("grp", "shard_0", "shard_1", "shard_2")
    )
    rows = P(SHARD, None, None)
    placed = (
        rows,
        rows,
        rows,
        P(SHARD),
        P("grp", SHARD),
        P("grp", SHARD, None, None),
        P(),
        P(None, GRP_SHARD),
        P(GRP_SHARD, None),
    ) + (P(),) * 9
    return jax.shard_map(
        body,
        mesh=finer,
        in_specs=placed,
        out_specs=(rows, rows, rows) + (P(),) * 9,
        check_vma=False,
    )
```

```python
import functools
import jax
import jax.numpy as jnp
from jax import lax
from jax.experimental import pallas as pl
from jax.experimental.pallas import tpu as pltpu
from jax.sharding import Mesh
from jax.sharding import PartitionSpec as P

TABLES = 26
CAP = 8
SHARD = ("shard_0", "shard_1", "shard_2")
GRP_SHARD = ("grp", "shard_0", "shard_1", "shard_2")
SUB = 8
LANE = 128
META_ROW = 2

beta_one = 0.9
beta_two = 0.999
corr_first = 1.0 - 0.9**10
corr_second = 1.0 - 0.999**10
adam_eps = 1e-06
decay_rate = 0.01
learn_rate = 0.1
ratio_eps = 1e-06

f32 = jnp.float32
bf16 = jnp.bfloat16
VMEM = pl.BlockSpec(memory_space=pltpu.VMEM)
SMEM = pl.BlockSpec(memory_space=pltpu.SMEM)
HBM = pl.BlockSpec(memory_space=pltpu.HBM)


LIMIT = pltpu.CompilerParams(vmem_limit_bytes=20 * 2**20)
WIDE = pltpu.CompilerParams(vmem_limit_bytes=53000 * 2**10)


def iota(shape, dim):
    return lax.broadcasted_iota(jnp.int32, shape, dim)


def subs():
    return iota((SUB, LANE), 0)


def turned(tile, rows):
    return pltpu.roll(tile, rows % SUB, 0) if rows % SUB else tile


def dot(a, b, ca, cb):
    return lax.dot_general(a, b, (((ca,), (cb,)), ((), ())), preferred_element_type=f32)


def log_two(n):
    return n.bit_length() - 1


def route_kernel(shards, blocks, groups, ids, block_slot, grads, out, wide):
    count = ids.shape[1]
    wide[...] = grads[...].astype(f32)
    for g in range(groups):
        rows = wide[pl.ds(g, count, stride=groups), :]
        out[g, 0 : count // SUB] = rows.reshape(count // SUB, SUB, LANE).astype(bf16)
    table_rows = block_slot.shape[0]
    high = ids[...] >> log_two(LANE)
    low = ids[...] & (LANE - 1)
    high_hot = iota((table_rows, count), 0) == high
    low_hot = iota((LANE, count), 0) == low
    slot = block_slot[...]
    one = high_hot.astype(f32).astype(bf16)
    owner_of = (slot >> log_two(blocks)).astype(f32).astype(bf16)
    local_of = (slot & (blocks - 1)).astype(f32).astype(bf16)
    owner = jnp.sum(jnp.where(low_hot, dot(owner_of, one, 0, 0), 0.0), axis=0, keepdims=True)
    local = jnp.sum(jnp.where(low_hot, dot(local_of, one, 0, 0), 0.0), axis=0, keepdims=True)
    owner_hot = iota((shards, count), 0).astype(f32) == owner
    before = (iota((count, count), 0) < iota((count, count), 1)).astype(f32).astype(bf16)
    rank = dot(owner_hot.astype(f32).astype(bf16), before, 1, 0)
    rank = jnp.sum(jnp.where(owner_hot, rank, 0.0), axis=0, keepdims=True)
    sub = iota((SUB, count), 0)
    tile = jnp.where(sub == 0, owner * CAP + rank, jnp.where(sub == 1, local + 1.0, 0.0))
    tile = tile.astype(bf16)
    for g in range(groups):
        out[g, count // SUB] = tile


def routed(ids, block_slot, grads, shards, blocks, groups):
    count = ids.shape[1]
    return pl.pallas_call(
        functools.partial(route_kernel, shards, blocks, groups),
        out_shape=jax.ShapeDtypeStruct((groups, count // SUB + 1, SUB, LANE), bf16),
        in_specs=[VMEM] * 3,
        out_specs=VMEM,
        scratch_shapes=[pltpu.VMEM(grads.shape, f32)],
        name="route",
    )(ids, block_slot, grads)


def bucket_kernel(shards, offset, recv, dense, out, rows_out, last_out, sem):
    groups = recv.shape[0]
    tiles = dense.shape[1]
    count = LANE
    copies = [
        pltpu.make_async_copy(
            dense.at[:, 0 : tiles - 1], out.at[:, groups : groups + tiles - 1], sem.at[groups]
        )
    ]
    copies[0].start()
    local_rows = jnp.zeros((shards, LANE), f32)
    for g in range(groups):
        tile = recv[g, count // SUB].astype(f32)
        place = tile[0:1].astype(jnp.int32)
        picker = (iota((shards * CAP, count), 0) == place).astype(f32).astype(bf16)
        rows = recv[g, 0 : count // SUB].astype(f32).reshape(count, LANE).astype(bf16)
        rows_out[:, g] = dot(picker, rows, 1, 0).reshape(shards, SUB, LANE).astype(bf16)
        copies.append(pltpu.make_async_copy(rows_out.at[:, g], out.at[:, g], sem.at[g]))
        copies[-1].start()
        owner = place >> log_two(CAP)
        lane = (place & (CAP - 1)) + g * CAP + offset[...]
        local = jnp.where(iota((shards, count), 0) == owner, tile[1:2], 0.0).astype(bf16)
        spot = (iota((LANE, count), 0) == lane).astype(f32).astype(bf16)
        local_rows += dot(local, spot, 1, 1)
    sub = subs()
    for s in range(shards):
        tile = dense[s, tiles - 1].astype(f32)
        tile = jnp.where(sub == META_ROW, local_rows[s : s + 1], tile)
        last_out[s] = tile.astype(bf16)
    copies.append(
        pltpu.make_async_copy(last_out, out.at[:, groups + tiles - 1], sem.at[groups + 1])
    )
    copies[-1].start()
    for c in copies:
        c.wait()


def bucketed(offset, recv, dense):
    shards, tiles = dense.shape[:2]
    groups = recv.shape[0]
    return pl.pallas_call(
        functools.partial(bucket_kernel, shards),
        out_shape=jax.ShapeDtypeStruct((shards, groups + tiles, SUB, LANE), bf16),
        in_specs=[VMEM] * 3,
        out_specs=HBM,
        scratch_shapes=[
            pltpu.VMEM((shards, groups, SUB, LANE), bf16),
            pltpu.VMEM((shards, SUB, LANE), bf16),
            pltpu.SemaphoreType.DMA((groups + 2,)),
        ],
        compiler_params=LIMIT,
        name="bucket",
    )(offset, recv, dense)


def act(half):
    bend = jnp.tanh(half)
    product = half * bend
    return (product + half).astype(bf16), (1.0 + bend) + (half - product * bend)


def tower_kernel(
    shards,
    parts,
    x_in,
    cot_in,
    w_one_in,
    w_two_in,
    w_three_in,
    out,
    x,
    cot,
    raw_one,
    raw_two,
    raw_three,
    w_one,
    w_two,
    w_two_t,
    w_three,
    g_one,
    g_two,
    g_three,
    sem,
    cot_sem,
):
    step = x.shape[1] // parts
    copies = [
        pltpu.make_async_copy(a, b, sem.at[i])
        for i, (a, b) in enumerate(
            ((w_one_in, raw_one), (x_in, x), (w_two_in, raw_two), (w_three_in, raw_three))
        )
    ]
    chunks = [
        pltpu.make_async_copy(
            cot_in.at[pl.ds(k * step, step), :], cot.at[pl.ds(k * step, step), :], cot_sem.at[k]
        )
        for k in range(parts)
    ]
    for c in copies + chunks:
        c.start()
    copies[0].wait()
    w_one[...] = (0.5 * raw_one[...]).astype(bf16)
    copies[1].wait()
    copies[2].wait()
    w_two[...] = (0.5 * raw_two[...]).astype(bf16)
    w_two_t[...] = (0.5 * raw_two[...]).T.astype(bf16)
    copies[3].wait()
    w_three[...] = (0.5 * raw_three[...]).astype(bf16)
    sums = None
    for k in range(parts):
        xs = x[:, k * step : (k + 1) * step]
        hidden_one, slope_one = act(dot(w_one[...], xs, 0, 0))
        hidden_two, slope_two = act(dot(w_two_t[...], hidden_one, 1, 0))
        chunks[k].wait()
        cots = cot[k * step : (k + 1) * step, :]
        three = dot(hidden_two, cots, 1, 0)
        back_two = (dot(w_three[...], cots, 1, 1) * slope_two).astype(bf16)
        two = dot(hidden_one, back_two, 1, 1)
        back_one = (dot(w_two[...], back_two, 1, 0) * slope_one).astype(bf16)
        one = dot(xs, back_one, 1, 1)
        if k == 0:
            g_one[0 : x.shape[0], :] = one
            g_two[...] = two
            g_three[...] = three
        else:
            g_one[0 : x.shape[0], :] += one
            g_two[...] += two
            g_three[...] += three
    g_one[x.shape[0] :, :] = jnp.zeros((g_one.shape[0] - x.shape[0], g_one.shape[1]), f32)
    rows_two = g_two.shape[0] // shards
    rows_three = g_three.shape[0] // shards
    halves = g_two.shape[1] // LANE
    for s in range(shards):
        at = 0
        for h in range(halves):
            for r in range(0, rows_two, SUB):
                out[s, at] = g_two[
                    s * rows_two + r : s * rows_two + r + SUB, h * LANE : (h + 1) * LANE
                ].astype(bf16)
                at += 1
        for r in range(0, rows_three, SUB):
            out[s, at] = g_three[s * rows_three + r : s * rows_three + r + SUB, :].astype(bf16)
            at += 1
        c, r = s // 4 // 2, s // 4 % 2
        tile = g_one[r * SUB : (r + 1) * SUB, c * LANE : (c + 1) * LANE]
        out[s, at] = turned(tile, -2 * (s % 4)).astype(bf16)


def tower(x, cot, w_one, w_two, w_three, shards, tiles, parts=2):
    din, samples = x.shape
    h_one, h_two = w_two.shape
    width = w_three.shape[1]
    macs = samples * (2 * din * h_one + 3 * h_one * h_two + 2 * h_two * width)
    return pl.pallas_call(
        functools.partial(tower_kernel, shards, parts),
        out_shape=jax.ShapeDtypeStruct((shards, tiles, SUB, LANE), bf16),
        in_specs=[HBM] * 5,
        out_specs=VMEM,
        scratch_shapes=[
            pltpu.VMEM(x.shape, bf16),
            pltpu.VMEM(cot.shape, bf16),
            pltpu.VMEM(w_one.shape, f32),
            pltpu.VMEM(w_two.shape, f32),
            pltpu.VMEM(w_three.shape, f32),
            pltpu.VMEM(w_one.shape, bf16),
            pltpu.VMEM(w_two.shape, bf16),
            pltpu.VMEM((h_two, h_one), bf16),
            pltpu.VMEM(w_three.shape, bf16),
            pltpu.VMEM((2 * SUB, h_one), f32),
            pltpu.VMEM((h_one, h_two), f32),
            pltpu.VMEM((h_two, width), f32),
            pltpu.SemaphoreType.DMA((4,)),
            pltpu.SemaphoreType.DMA((parts,)),
        ],
        cost_estimate=pl.CostEstimate(
            flops=2 * macs, bytes_accessed=4 * samples * width, transcendentals=samples * h_one
        ),
        compiler_params=pltpu.CompilerParams(vmem_limit_bytes=54000 * 2**10),
        name="tower",
    )(x, cot, w_one, w_two, w_three)


def lamb_step(weight, first_in, second_in, gradient):
    first_out = beta_one * first_in + (1.0 - beta_one) * gradient
    second_out = beta_two * second_in + (1.0 - beta_two) * gradient * gradient
    update = (first_out * (1.0 / corr_first)) / (
        jnp.sqrt(second_out * (1.0 / corr_second)) + adam_eps
    ) + decay_rate * weight
    return update, first_out, second_out


def with_sums(tile, rows):
    sub = subs()
    for i, value in enumerate(rows):
        high = value.astype(bf16).astype(f32)
        tile = jnp.where(sub == 2 * i + 2, high, tile)
        tile = jnp.where(sub == 2 * i + 3, value - high, tile)
    return tile


def sums_in(tile):
    return [tile[i : i + 1] + tile[i + 1 : i + 2] for i in (2, 4)]


def table_hot(slot_table):
    return slot_table[...] == iota((slot_table.shape[0], LANE), 1)


def own_kernel(tiles, slot_table, recv, table, first, second, out, hit_out):
    shards = recv.shape[0]
    groups = out.shape[0]
    blocks = slot_table.shape[0]
    total = jnp.zeros((blocks, LANE), f32)
    hits = jnp.zeros((blocks, LANE), f32)
    slot = iota((blocks, LANE), 0) + 1
    for s in range(0, shards, 2):
        tile = recv[s, groups + tiles - 1].astype(f32) + recv[s + 1, groups + tiles - 1].astype(f32)
        place = tile[META_ROW : META_ROW + 1]
        match = (slot == place.astype(jnp.int32)).astype(f32)
        rows = recv[s : s + 2, 0:groups].astype(f32).reshape(LANE, LANE).astype(bf16)
        total += dot(match.astype(bf16), rows, 1, 0)
        hits += match
    hits = dot(hits.astype(bf16), jnp.ones((LANE, LANE), bf16), 1, 0)
    hit_out[...] = hits
    sent = total.reshape(blocks // SUB, SUB, LANE).astype(bf16)
    weight = table[...]
    update, unused, unused_too = lamb_step(
        weight, first[...], second[...], sent.astype(f32).reshape(blocks, LANE)
    )
    update = jnp.where(hits > 0.5, update, 0.0)
    hot = table_hot(slot_table)
    sums = []
    for v in (weight, update):
        row = jnp.sum(v * v, axis=1, keepdims=True)
        sums.append(jnp.sum(jnp.where(hot, row, 0.0), axis=0, keepdims=True))
    dense = recv[0, groups:].astype(f32)
    for s in range(1, shards):
        dense = dense + recv[s, groups:].astype(f32)
    mixed = with_sums(dense[tiles - 1], sums).astype(bf16)
    dense = dense[: tiles - 1].astype(bf16)
    for g in range(groups):
        out[g, 0 : blocks // SUB] = sent
        out[g, blocks // SUB : blocks // SUB + tiles - 1] = dense
        out[g, blocks // SUB + tiles - 1] = mixed


def owned(slot_table, recv, table, first, second, groups, tiles):
    blocks = slot_table.shape[0]
    return pl.pallas_call(
        functools.partial(own_kernel, tiles),
        out_shape=(
            jax.ShapeDtypeStruct((groups, blocks // SUB + tiles, SUB, LANE), bf16),
            jax.ShapeDtypeStruct((blocks, LANE), f32),
        ),
        in_specs=[VMEM] * 5,
        out_specs=(VMEM,) * 2,
        compiler_params=LIMIT,
        name="own",
    )(slot_table, recv, table, first, second)


def pack_kernel(tiles, recv, out):
    groups = recv.shape[0]
    start = recv.shape[1] - tiles
    lines = recv[0, start:].astype(f32)
    for g in range(1, groups):
        lines = lines + recv[g, start:].astype(f32)
    dense = lines[: tiles - 1].astype(bf16)
    mixed = lines[tiles - 1]
    mixed = with_sums(mixed, sums_in(mixed)).astype(bf16)
    for s in range(out.shape[0]):
        out[s, 0 : tiles - 1] = dense
        out[s, tiles - 1] = mixed


def packed(recv, shards, tiles):
    return pl.pallas_call(
        functools.partial(pack_kernel, tiles),
        out_shape=jax.ShapeDtypeStruct((shards, tiles, SUB, LANE), bf16),
        in_specs=[VMEM],
        out_specs=VMEM,
        compiler_params=LIMIT,
        name="pack",
    )(recv)


def slots_kernel(
    recv,
    hit,
    table_in,
    first_in,
    second_in,
    new_first_out,
    new_second_out,
    update,
    table,
    first,
    second,
    sem,
    out_sem,
):
    groups = recv.shape[0]
    blocks = hit.shape[0]
    copies = [
        pltpu.make_async_copy(a, b, sem.at[i])
        for i, (a, b) in enumerate(((table_in, table), (first_in, first), (second_in, second)))
    ]
    for c in copies:
        c.start()
    touched = hit[...] > 0.5
    for c in copies:
        c.wait()
    for g in range(groups):
        column = pl.ds(g, blocks, stride=groups)
        grad = recv[g, 0 : blocks // SUB].astype(f32).reshape(blocks, LANE)
        old_first, old_second = first[column, :], second[column, :]
        change, first_out, second_out = lamb_step(table[column, :], old_first, old_second, grad)
        first[column, :] = jnp.where(touched, first_out, old_first)
        second[column, :] = jnp.where(touched, second_out, old_second)
        update[column, :] = jnp.where(touched, change, 0.0)
    leave = [
        pltpu.make_async_copy(a, b, out_sem.at[i])
        for i, (a, b) in enumerate(((first, new_first_out), (second, new_second_out)))
    ]
    for c in leave:
        c.start()
    for c in leave:
        c.wait()


def slots(recv, hit, table, first, second):
    shape = jax.ShapeDtypeStruct(table.shape, f32)
    return pl.pallas_call(
        slots_kernel,
        out_shape=(shape,) * 3,
        in_specs=[VMEM] * 2 + [HBM] * 3,
        out_specs=(HBM,) * 2 + (VMEM,),
        scratch_shapes=[pltpu.VMEM(table.shape, f32)] * 3
        + [pltpu.SemaphoreType.DMA((3,)), pltpu.SemaphoreType.DMA((2,))],
        cost_estimate=pl.CostEstimate(
            flops=2000 * table.size, bytes_accessed=24 * table.size, transcendentals=table.size
        ),
        compiler_params=WIDE,
        name="slots",
    )(recv, hit, table, first, second)


def lamb_whole(weight, first_in, second_in, gradient):
    update, first_out, second_out = lamb_step(weight, first_in, second_in, gradient)
    ratio = jnp.sqrt(jnp.sum(weight * weight, keepdims=True)) / (
        jnp.sqrt(jnp.sum(update * update, keepdims=True)) + ratio_eps
    )
    return (weight - learn_rate * ratio * update, first_out, second_out)


def last_kernel(slot_table, recv, table, update, *refs):
    ins, outs, scratch = refs[:9], refs[9:19], refs[19:]
    held, made, (g_one, g_two, g_three, sem, out_sem) = scratch[:9], scratch[9:19], scratch[19:]
    arrive = [pltpu.make_async_copy(a, b, sem.at[i]) for i, (a, b) in enumerate(zip(ins, held))]
    leave = [pltpu.make_async_copy(a, b, out_sem.at[i]) for i, (a, b) in enumerate(zip(made, outs))]
    for i in (1, 4, 7, 2, 5, 8, 0, 3, 6):
        arrive[i].start()
    shards, tiles = recv.shape[:2]
    pieces = recv[0, tiles - 1].astype(f32)
    for s in range(1, shards):
        pieces = pieces + recv[s, tiles - 1].astype(f32)
    weight_sq, update_sq = sums_in(pieces)
    ratio = learn_rate * (jnp.sqrt(weight_sq) / (jnp.sqrt(update_sq) + ratio_eps))
    ratio = jnp.sum(jnp.where(table_hot(slot_table), ratio, 0.0), axis=1, keepdims=True)
    blocks = slot_table.shape[0]
    groups = table.shape[0] // blocks
    for g in range(groups):
        column = pl.ds(g, blocks, stride=groups)
        made[0][column, :] = table[column, :] - ratio * update[column, :]
    leave[0].start()
    pair = subs() // 2
    rows_two = g_two.shape[0] // shards
    rows_three = g_three.shape[0] // shards
    halves = g_two.shape[1] // LANE
    for s in range(shards):
        at = 0
        for h in range(halves):
            for r in range(0, rows_two, SUB):
                g_two[s * rows_two + r : s * rows_two + r + SUB, h * LANE : (h + 1) * LANE] = recv[
                    s, at
                ].astype(f32)
                at += 1
        for r in range(0, rows_three, SUB):
            g_three[s * rows_three + r : s * rows_three + r + SUB, :] = recv[s, at].astype(f32)
            at += 1
    for k in range(shards // 4):
        tile = jnp.zeros((SUB, LANE), f32)
        for a in range(4):
            piece = turned(recv[4 * k + a, tiles - 1].astype(f32), 2 * a)
            tile = jnp.where(pair == a, piece, tile)
        c, r = k // 2, k % 2
        g_one[r * SUB : (r + 1) * SUB, c * LANE : (c + 1) * LANE] = tile

    def dense(n, gradient):
        for i in (n, 3 + n, 6 + n):
            arrive[i].wait()
        weight, first, second = held[n], held[3 + n], held[6 + n]
        made[1 + n][...], made[4 + n][...], made[7 + n][...] = lamb_whole(
            weight[...], first[...], second[...], gradient[0 : weight.shape[0], :]
        )
        for i in (1 + n, 4 + n, 7 + n):
            leave[i].start()

    dense(1, g_two)
    dense(2, g_three)
    dense(0, g_one)
    for c in leave:
        c.wait()


def last(slot_table, recv, table, update, weights):
    outs = (table,) + weights
    return pl.pallas_call(
        last_kernel,
        out_shape=tuple(jax.ShapeDtypeStruct(a.shape, f32) for a in outs),
        in_specs=[VMEM] * 4 + [HBM] * 9,
        out_specs=(HBM,) * 10,
        scratch_shapes=[pltpu.VMEM(a.shape, f32) for a in weights + outs]
        + [
            pltpu.VMEM((2 * SUB, weights[0].shape[1]), f32),
            pltpu.VMEM(weights[1].shape, f32),
            pltpu.VMEM(weights[2].shape, f32),
            pltpu.SemaphoreType.DMA((len(weights),)),
            pltpu.SemaphoreType.DMA((len(outs),)),
        ],
        compiler_params=WIDE,
        name="last",
    )(slot_table, recv, table, update, *weights)


def exchange(value, axis):
    return lax.all_to_all(value, axis, split_axis=0, concat_axis=0, tiled=True)


def body(
    table,
    table_first,
    table_second,
    slot_table,
    touched,
    emb_grads,
    block_slot,
    dense_x,
    dense_cot,
    w_one,
    w_two,
    w_three,
    first_one,
    first_two,
    first_three,
    second_one,
    second_two,
    second_three,
):
    shards = lax.axis_size(SHARD)
    groups = lax.axis_size("grp")
    blocks = table.shape[0]
    tiles = (w_two.size + w_three.size) // (shards * SUB * LANE) + 1
    group = lax.axis_index("grp")
    offset = jnp.full((1, LANE), lax.axis_index(SHARD[2]) * (LANE // 2), jnp.int32)
    column = lambda a: lax.dynamic_index_in_dim(a, group, 1, keepdims=False)
    flat = lambda a: a.reshape(-1, LANE)
    slot_column = slot_table[:, None]

    recv = exchange(
        routed(touched, flat(block_slot), flat(emb_grads), shards, blocks, groups), "grp"
    )
    dense = tower(dense_x, dense_cot, w_one, w_two, w_three, shards, tiles)
    recv = exchange(bucketed(offset, recv, dense), SHARD)
    rows = flat(table), flat(table_first), flat(table_second)
    columns = [column(a) for a in (table, table_first, table_second)]
    mine, hit = owned(slot_column, recv, *columns, groups, tiles)
    whole = exchange(mine, "grp")
    spread = exchange(packed(whole, shards, tiles), SHARD)
    new_first, new_second, update = slots(whole, hit, *rows)
    weights = (
        w_one,
        w_two,
        w_three,
        first_one,
        first_two,
        first_three,
        second_one,
        second_two,
        second_three,
    )
    new_table, *rest = last(slot_column, spread, rows[0], update, weights)
    back = [a.reshape(table.shape) for a in (new_table, new_first, new_second)]
    return (*back, *rest)


def solution(mesh):
    finer = Mesh(
        mesh.devices.reshape(mesh.shape["grp"], 4, 4, 2), ("grp", "shard_0", "shard_1", "shard_2")
    )
    rows = P(SHARD, None, None)
    placed = (
        rows,
        rows,
        rows,
        P(SHARD),
        P("grp", SHARD),
        P("grp", SHARD, None, None),
        P(),
        P(None, GRP_SHARD),
        P(GRP_SHARD, None),
    ) + (P(),) * 9
    return jax.shard_map(
        body,
        mesh=finer,
        in_specs=placed,
        out_specs=(rows, rows, rows) + (P(),) * 9,
        check_vma=False,
    )
```

```python
import functools
import jax
import jax.numpy as jnp
from jax import lax
from jax.experimental import pallas as pl
from jax.experimental.pallas import tpu as pltpu
from jax.sharding import Mesh
from jax.sharding import PartitionSpec as P

TABLES = 26
CAP = 8
SHARD = ("shard_0", "shard_1", "shard_2")
GRP_SHARD = ("grp", "shard_0", "shard_1", "shard_2")
SUB = 8
LANE = 128
META_ROW = 2

beta_one = 0.9
beta_two = 0.999
corr_first = 1.0 - 0.9**10
corr_second = 1.0 - 0.999**10
adam_eps = 1e-06
decay_rate = 0.01
learn_rate = 0.1
ratio_eps = 1e-06

f32 = jnp.float32
bf16 = jnp.bfloat16
VMEM = pl.BlockSpec(memory_space=pltpu.VMEM)
SMEM = pl.BlockSpec(memory_space=pltpu.SMEM)
HBM = pl.BlockSpec(memory_space=pltpu.HBM)


LIMIT = pltpu.CompilerParams(vmem_limit_bytes=20 * 2**20)
WIDE = pltpu.CompilerParams(vmem_limit_bytes=53000 * 2**10)


def iota(shape, dim):
    return lax.broadcasted_iota(jnp.int32, shape, dim)


def subs():
    return iota((SUB, LANE), 0)


def turned(tile, rows):
    return pltpu.roll(tile, rows % SUB, 0) if rows % SUB else tile


def dot(a, b, ca, cb):
    return lax.dot_general(a, b, (((ca,), (cb,)), ((), ())), preferred_element_type=f32)


def log_two(n):
    return n.bit_length() - 1


def route_kernel(shards, blocks, groups, ids, block_slot, grads, out, wide):
    count = ids.shape[1]
    wide[...] = grads[...].astype(f32)
    for g in range(groups):
        rows = wide[pl.ds(g, count, stride=groups), :]
        out[g, 0 : count // SUB] = rows.reshape(count // SUB, SUB, LANE).astype(bf16)
    table_rows = block_slot.shape[0]
    high = ids[...] >> log_two(LANE)
    low = ids[...] & (LANE - 1)
    high_hot = iota((table_rows, count), 0) == high
    low_hot = iota((LANE, count), 0) == low
    slot = block_slot[...]
    one = high_hot.astype(f32).astype(bf16)
    owner_of = (slot >> log_two(blocks)).astype(f32).astype(bf16)
    local_of = (slot & (blocks - 1)).astype(f32).astype(bf16)
    owner = jnp.sum(jnp.where(low_hot, dot(owner_of, one, 0, 0), 0.0), axis=0, keepdims=True)
    local = jnp.sum(jnp.where(low_hot, dot(local_of, one, 0, 0), 0.0), axis=0, keepdims=True)
    owner_hot = iota((shards, count), 0).astype(f32) == owner
    before = (iota((count, count), 0) < iota((count, count), 1)).astype(f32).astype(bf16)
    rank = dot(owner_hot.astype(f32).astype(bf16), before, 1, 0)
    rank = jnp.sum(jnp.where(owner_hot, rank, 0.0), axis=0, keepdims=True)
    sub = iota((SUB, count), 0)
    tile = jnp.where(sub == 0, owner * CAP + rank, jnp.where(sub == 1, local + 1.0, 0.0))
    tile = tile.astype(bf16)
    for g in range(groups):
        out[g, count // SUB] = tile


def routed(ids, block_slot, grads, shards, blocks, groups):
    count = ids.shape[1]
    return pl.pallas_call(
        functools.partial(route_kernel, shards, blocks, groups),
        out_shape=jax.ShapeDtypeStruct((groups, count // SUB + 1, SUB, LANE), bf16),
        in_specs=[VMEM] * 3,
        out_specs=VMEM,
        scratch_shapes=[pltpu.VMEM(grads.shape, f32)],
        name="route",
    )(ids, block_slot, grads)


def bucket_kernel(shards, offset, recv, dense, out, rows_out, last_out, sem):
    groups = recv.shape[0]
    tiles = dense.shape[1]
    count = LANE
    copies = [
        pltpu.make_async_copy(
            dense.at[:, 0 : tiles - 1], out.at[:, groups : groups + tiles - 1], sem.at[groups]
        )
    ]
    copies[0].start()
    local_rows = jnp.zeros((shards, LANE), f32)
    for g in range(groups):
        tile = recv[g, count // SUB].astype(f32)
        place = tile[0:1].astype(jnp.int32)
        picker = (iota((shards * CAP, count), 0) == place).astype(f32).astype(bf16)
        rows = recv[g, 0 : count // SUB].astype(f32).reshape(count, LANE).astype(bf16)
        rows_out[:, g] = dot(picker, rows, 1, 0).reshape(shards, SUB, LANE).astype(bf16)
        copies.append(pltpu.make_async_copy(rows_out.at[:, g], out.at[:, g], sem.at[g]))
        copies[-1].start()
        owner = place >> log_two(CAP)
        lane = (place & (CAP - 1)) + g * CAP + offset[...]
        local = jnp.where(iota((shards, count), 0) == owner, tile[1:2], 0.0).astype(bf16)
        spot = (iota((LANE, count), 0) == lane).astype(f32).astype(bf16)
        local_rows += dot(local, spot, 1, 1)
    sub = subs()
    for s in range(shards):
        tile = dense[s, tiles - 1].astype(f32)
        tile = jnp.where(sub == META_ROW, local_rows[s : s + 1], tile)
        last_out[s] = tile.astype(bf16)
    copies.append(
        pltpu.make_async_copy(last_out, out.at[:, groups + tiles - 1], sem.at[groups + 1])
    )
    copies[-1].start()
    for c in copies:
        c.wait()


def bucketed(offset, recv, dense):
    shards, tiles = dense.shape[:2]
    groups = recv.shape[0]
    return pl.pallas_call(
        functools.partial(bucket_kernel, shards),
        out_shape=jax.ShapeDtypeStruct((shards, groups + tiles, SUB, LANE), bf16),
        in_specs=[VMEM] * 3,
        out_specs=HBM,
        scratch_shapes=[
            pltpu.VMEM((shards, groups, SUB, LANE), bf16),
            pltpu.VMEM((shards, SUB, LANE), bf16),
            pltpu.SemaphoreType.DMA((groups + 2,)),
        ],
        compiler_params=LIMIT,
        name="bucket",
    )(offset, recv, dense)


def act(half):
    bend = jnp.tanh(half)
    product = half * bend
    return (product + half).astype(bf16), (1.0 + bend) + (half - product * bend)


def tower_kernel(
    shards,
    parts,
    x_in,
    cot_in,
    w_one_in,
    w_two_in,
    w_three_in,
    out,
    x,
    cot,
    raw_one,
    raw_two,
    raw_three,
    w_one,
    w_two,
    w_two_t,
    w_three,
    g_one,
    g_two,
    g_three,
    sem,
    cot_sem,
):
    step = x.shape[1] // parts
    copies = [
        pltpu.make_async_copy(a, b, sem.at[i])
        for i, (a, b) in enumerate(
            ((w_one_in, raw_one), (x_in, x), (w_two_in, raw_two), (w_three_in, raw_three))
        )
    ]
    chunks = [
        pltpu.make_async_copy(
            cot_in.at[pl.ds(k * step, step), :], cot.at[pl.ds(k * step, step), :], cot_sem.at[k]
        )
        for k in range(parts)
    ]
    for c in copies + chunks:
        c.start()
    copies[0].wait()
    w_one[...] = (0.5 * raw_one[...]).astype(bf16)
    copies[1].wait()
    copies[2].wait()
    w_two[...] = (0.5 * raw_two[...]).astype(bf16)
    w_two_t[...] = (0.5 * raw_two[...]).T.astype(bf16)
    copies[3].wait()
    w_three[...] = (0.5 * raw_three[...]).astype(bf16)
    sums = None
    for k in range(parts):
        xs = x[:, k * step : (k + 1) * step]
        if k == 0:
            hidden_one, slope_one = act(dot(w_one[...], xs, 0, 0))
        else:
            hidden_one, slope_one = ahead
        hidden_two, slope_two = act(dot(w_two_t[...], hidden_one, 1, 0))
        chunks[k].wait()
        cots = cot[k * step : (k + 1) * step, :]
        if k + 1 < parts:
            ahead = act(dot(w_one[...], x[:, (k + 1) * step : (k + 2) * step], 0, 0))
        three = dot(hidden_two, cots, 1, 0)
        back_two = (dot(w_three[...], cots, 1, 1) * slope_two).astype(bf16)
        two = dot(hidden_one, back_two, 1, 1)
        back_one = (dot(w_two[...], back_two, 1, 0) * slope_one).astype(bf16)
        one = dot(xs, back_one, 1, 1)
        if k == 0:
            g_one[0 : x.shape[0], :] = one
            g_two[...] = two
            g_three[...] = three
        else:
            g_one[0 : x.shape[0], :] += one
            g_two[...] += two
            g_three[...] += three
    g_one[x.shape[0] :, :] = jnp.zeros((g_one.shape[0] - x.shape[0], g_one.shape[1]), f32)
    rows_two = g_two.shape[0] // shards
    rows_three = g_three.shape[0] // shards
    halves = g_two.shape[1] // LANE
    for s in range(shards):
        at = 0
        for h in range(halves):
            for r in range(0, rows_two, SUB):
                out[s, at] = g_two[
                    s * rows_two + r : s * rows_two + r + SUB, h * LANE : (h + 1) * LANE
                ].astype(bf16)
                at += 1
        for r in range(0, rows_three, SUB):
            out[s, at] = g_three[s * rows_three + r : s * rows_three + r + SUB, :].astype(bf16)
            at += 1
        c, r = s // 4 // 2, s // 4 % 2
        tile = g_one[r * SUB : (r + 1) * SUB, c * LANE : (c + 1) * LANE]
        out[s, at] = turned(tile, -2 * (s % 4)).astype(bf16)


def tower(x, cot, w_one, w_two, w_three, shards, tiles, parts=2):
    din, samples = x.shape
    h_one, h_two = w_two.shape
    width = w_three.shape[1]
    macs = samples * (2 * din * h_one + 3 * h_one * h_two + 2 * h_two * width)
    return pl.pallas_call(
        functools.partial(tower_kernel, shards, parts),
        out_shape=jax.ShapeDtypeStruct((shards, tiles, SUB, LANE), bf16),
        in_specs=[HBM] * 5,
        out_specs=VMEM,
        scratch_shapes=[
            pltpu.VMEM(x.shape, bf16),
            pltpu.VMEM(cot.shape, bf16),
            pltpu.VMEM(w_one.shape, f32),
            pltpu.VMEM(w_two.shape, f32),
            pltpu.VMEM(w_three.shape, f32),
            pltpu.VMEM(w_one.shape, bf16),
            pltpu.VMEM(w_two.shape, bf16),
            pltpu.VMEM((h_two, h_one), bf16),
            pltpu.VMEM(w_three.shape, bf16),
            pltpu.VMEM((2 * SUB, h_one), f32),
            pltpu.VMEM((h_one, h_two), f32),
            pltpu.VMEM((h_two, width), f32),
            pltpu.SemaphoreType.DMA((4,)),
            pltpu.SemaphoreType.DMA((parts,)),
        ],
        cost_estimate=pl.CostEstimate(
            flops=2 * macs, bytes_accessed=4 * samples * width, transcendentals=samples * h_one
        ),
        compiler_params=pltpu.CompilerParams(vmem_limit_bytes=54000 * 2**10),
        name="tower",
    )(x, cot, w_one, w_two, w_three)


def lamb_step(weight, first_in, second_in, gradient):
    first_out = beta_one * first_in + (1.0 - beta_one) * gradient
    second_out = beta_two * second_in + (1.0 - beta_two) * gradient * gradient
    update = (first_out * (1.0 / corr_first)) / (
        jnp.sqrt(second_out * (1.0 / corr_second)) + adam_eps
    ) + decay_rate * weight
    return update, first_out, second_out


def with_sums(tile, rows):
    sub = subs()
    for i, value in enumerate(rows):
        high = value.astype(bf16).astype(f32)
        tile = jnp.where(sub == 2 * i + 2, high, tile)
        tile = jnp.where(sub == 2 * i + 3, value - high, tile)
    return tile


def sums_in(tile):
    return [tile[i : i + 1] + tile[i + 1 : i + 2] for i in (2, 4)]


def table_hot(slot_table):
    return slot_table[...] == iota((slot_table.shape[0], LANE), 1)


def own_kernel(tiles, slot_table, recv, table, first, second, out, hit_out):
    shards = recv.shape[0]
    groups = out.shape[0]
    blocks = slot_table.shape[0]
    total = jnp.zeros((blocks, LANE), f32)
    hits = jnp.zeros((blocks, LANE), f32)
    slot = iota((blocks, LANE), 0) + 1
    for s in range(0, shards, 2):
        tile = recv[s, groups + tiles - 1].astype(f32) + recv[s + 1, groups + tiles - 1].astype(f32)
        place = tile[META_ROW : META_ROW + 1]
        match = (slot == place.astype(jnp.int32)).astype(f32)
        rows = recv[s : s + 2, 0:groups].astype(f32).reshape(LANE, LANE).astype(bf16)
        total += dot(match.astype(bf16), rows, 1, 0)
        hits += match
    hits = dot(hits.astype(bf16), jnp.ones((LANE, LANE), bf16), 1, 0)
    hit_out[...] = hits
    sent = total.reshape(blocks // SUB, SUB, LANE).astype(bf16)
    weight = table[...]
    update, unused, unused_too = lamb_step(
        weight, first[...], second[...], sent.astype(f32).reshape(blocks, LANE)
    )
    update = jnp.where(hits > 0.5, update, 0.0)
    hot = table_hot(slot_table)
    sums = []
    for v in (weight, update):
        row = jnp.sum(v * v, axis=1, keepdims=True)
        sums.append(jnp.sum(jnp.where(hot, row, 0.0), axis=0, keepdims=True))
    dense = recv[0, groups:].astype(f32)
    for s in range(1, shards):
        dense = dense + recv[s, groups:].astype(f32)
    mixed = with_sums(dense[tiles - 1], sums).astype(bf16)
    dense = dense[: tiles - 1].astype(bf16)
    for g in range(groups):
        out[g, 0 : blocks // SUB] = sent
        out[g, blocks // SUB : blocks // SUB + tiles - 1] = dense
        out[g, blocks // SUB + tiles - 1] = mixed


def owned(slot_table, recv, table, first, second, groups, tiles):
    blocks = slot_table.shape[0]
    return pl.pallas_call(
        functools.partial(own_kernel, tiles),
        out_shape=(
            jax.ShapeDtypeStruct((groups, blocks // SUB + tiles, SUB, LANE), bf16),
            jax.ShapeDtypeStruct((blocks, LANE), f32),
        ),
        in_specs=[VMEM] * 5,
        out_specs=(VMEM,) * 2,
        compiler_params=LIMIT,
        name="own",
    )(slot_table, recv, table, first, second)


def pack_kernel(tiles, recv, out):
    groups = recv.shape[0]
    start = recv.shape[1] - tiles
    lines = recv[0, start:].astype(f32)
    for g in range(1, groups):
        lines = lines + recv[g, start:].astype(f32)
    dense = lines[: tiles - 1].astype(bf16)
    mixed = lines[tiles - 1]
    mixed = with_sums(mixed, sums_in(mixed)).astype(bf16)
    for s in range(out.shape[0]):
        out[s, 0 : tiles - 1] = dense
        out[s, tiles - 1] = mixed


def packed(recv, shards, tiles):
    return pl.pallas_call(
        functools.partial(pack_kernel, tiles),
        out_shape=jax.ShapeDtypeStruct((shards, tiles, SUB, LANE), bf16),
        in_specs=[VMEM],
        out_specs=VMEM,
        compiler_params=LIMIT,
        name="pack",
    )(recv)


def slots_kernel(
    recv,
    hit,
    table_in,
    first_in,
    second_in,
    new_first_out,
    new_second_out,
    update,
    table,
    first,
    second,
    sem,
    out_sem,
):
    groups = recv.shape[0]
    blocks = hit.shape[0]
    copies = [
        pltpu.make_async_copy(a, b, sem.at[i])
        for i, (a, b) in enumerate(((table_in, table), (first_in, first), (second_in, second)))
    ]
    for c in copies:
        c.start()
    touched = hit[...] > 0.5
    for c in copies:
        c.wait()
    for g in range(groups):
        column = pl.ds(g, blocks, stride=groups)
        grad = recv[g, 0 : blocks // SUB].astype(f32).reshape(blocks, LANE)
        old_first, old_second = first[column, :], second[column, :]
        change, first_out, second_out = lamb_step(table[column, :], old_first, old_second, grad)
        first[column, :] = jnp.where(touched, first_out, old_first)
        second[column, :] = jnp.where(touched, second_out, old_second)
        update[column, :] = jnp.where(touched, change, 0.0)
    leave = [
        pltpu.make_async_copy(a, b, out_sem.at[i])
        for i, (a, b) in enumerate(((first, new_first_out), (second, new_second_out)))
    ]
    for c in leave:
        c.start()
    for c in leave:
        c.wait()


def slots(recv, hit, table, first, second):
    shape = jax.ShapeDtypeStruct(table.shape, f32)
    return pl.pallas_call(
        slots_kernel,
        out_shape=(shape,) * 3,
        in_specs=[VMEM] * 2 + [HBM] * 3,
        out_specs=(HBM,) * 2 + (VMEM,),
        scratch_shapes=[pltpu.VMEM(table.shape, f32)] * 3
        + [pltpu.SemaphoreType.DMA((3,)), pltpu.SemaphoreType.DMA((2,))],
        cost_estimate=pl.CostEstimate(
            flops=2000 * table.size, bytes_accessed=24 * table.size, transcendentals=table.size
        ),
        compiler_params=WIDE,
        name="slots",
    )(recv, hit, table, first, second)


def lamb_whole(weight, first_in, second_in, gradient):
    update, first_out, second_out = lamb_step(weight, first_in, second_in, gradient)
    ratio = jnp.sqrt(jnp.sum(weight * weight, keepdims=True)) / (
        jnp.sqrt(jnp.sum(update * update, keepdims=True)) + ratio_eps
    )
    return (weight - learn_rate * ratio * update, first_out, second_out)


def last_kernel(slot_table, recv, table, update, *refs):
    ins, outs, scratch = refs[:9], refs[9:19], refs[19:]
    held, made, (g_one, g_two, g_three, sem, out_sem) = scratch[:9], scratch[9:19], scratch[19:]
    arrive = [pltpu.make_async_copy(a, b, sem.at[i]) for i, (a, b) in enumerate(zip(ins, held))]
    leave = [pltpu.make_async_copy(a, b, out_sem.at[i]) for i, (a, b) in enumerate(zip(made, outs))]
    for i in (1, 4, 7, 2, 5, 8, 0, 3, 6):
        arrive[i].start()
    shards, tiles = recv.shape[:2]
    pieces = recv[0, tiles - 1].astype(f32)
    for s in range(1, shards):
        pieces = pieces + recv[s, tiles - 1].astype(f32)
    weight_sq, update_sq = sums_in(pieces)
    ratio = learn_rate * (jnp.sqrt(weight_sq) / (jnp.sqrt(update_sq) + ratio_eps))
    ratio = jnp.sum(jnp.where(table_hot(slot_table), ratio, 0.0), axis=1, keepdims=True)
    blocks = slot_table.shape[0]
    groups = table.shape[0] // blocks
    for g in range(groups):
        column = pl.ds(g, blocks, stride=groups)
        made[0][column, :] = table[column, :] - ratio * update[column, :]
    leave[0].start()
    pair = subs() // 2
    rows_two = g_two.shape[0] // shards
    rows_three = g_three.shape[0] // shards
    halves = g_two.shape[1] // LANE
    for s in range(shards):
        at = 0
        for h in range(halves):
            for r in range(0, rows_two, SUB):
                g_two[s * rows_two + r : s * rows_two + r + SUB, h * LANE : (h + 1) * LANE] = recv[
                    s, at
                ].astype(f32)
                at += 1
        for r in range(0, rows_three, SUB):
            g_three[s * rows_three + r : s * rows_three + r + SUB, :] = recv[s, at].astype(f32)
            at += 1
    for k in range(shards // 4):
        tile = jnp.zeros((SUB, LANE), f32)
        for a in range(4):
            piece = turned(recv[4 * k + a, tiles - 1].astype(f32), 2 * a)
            tile = jnp.where(pair == a, piece, tile)
        c, r = k // 2, k % 2
        g_one[r * SUB : (r + 1) * SUB, c * LANE : (c + 1) * LANE] = tile

    def dense(n, gradient):
        for i in (n, 3 + n, 6 + n):
            arrive[i].wait()
        weight, first, second = held[n], held[3 + n], held[6 + n]
        made[1 + n][...], made[4 + n][...], made[7 + n][...] = lamb_whole(
            weight[...], first[...], second[...], gradient[0 : weight.shape[0], :]
        )
        for i in (1 + n, 4 + n, 7 + n):
            leave[i].start()

    dense(1, g_two)
    dense(2, g_three)
    dense(0, g_one)
    for c in leave:
        c.wait()


def last(slot_table, recv, table, update, weights):
    outs = (table,) + weights
    return pl.pallas_call(
        last_kernel,
        out_shape=tuple(jax.ShapeDtypeStruct(a.shape, f32) for a in outs),
        in_specs=[VMEM] * 4 + [HBM] * 9,
        out_specs=(HBM,) * 10,
        scratch_shapes=[pltpu.VMEM(a.shape, f32) for a in weights + outs]
        + [
            pltpu.VMEM((2 * SUB, weights[0].shape[1]), f32),
            pltpu.VMEM(weights[1].shape, f32),
            pltpu.VMEM(weights[2].shape, f32),
            pltpu.SemaphoreType.DMA((len(weights),)),
            pltpu.SemaphoreType.DMA((len(outs),)),
        ],
        compiler_params=WIDE,
        name="last",
    )(slot_table, recv, table, update, *weights)


def exchange(value, axis):
    return lax.all_to_all(value, axis, split_axis=0, concat_axis=0, tiled=True)


def body(
    table,
    table_first,
    table_second,
    slot_table,
    touched,
    emb_grads,
    block_slot,
    dense_x,
    dense_cot,
    w_one,
    w_two,
    w_three,
    first_one,
    first_two,
    first_three,
    second_one,
    second_two,
    second_three,
):
    shards = lax.axis_size(SHARD)
    groups = lax.axis_size("grp")
    blocks = table.shape[0]
    tiles = (w_two.size + w_three.size) // (shards * SUB * LANE) + 1
    group = lax.axis_index("grp")
    offset = jnp.full((1, LANE), lax.axis_index(SHARD[2]) * (LANE // 2), jnp.int32)
    column = lambda a: lax.dynamic_index_in_dim(a, group, 1, keepdims=False)
    flat = lambda a: a.reshape(-1, LANE)
    slot_column = slot_table[:, None]

    recv = exchange(
        routed(touched, flat(block_slot), flat(emb_grads), shards, blocks, groups), "grp"
    )
    dense = tower(dense_x, dense_cot, w_one, w_two, w_three, shards, tiles)
    recv = exchange(bucketed(offset, recv, dense), SHARD)
    rows = flat(table), flat(table_first), flat(table_second)
    columns = [column(a) for a in (table, table_first, table_second)]
    mine, hit = owned(slot_column, recv, *columns, groups, tiles)
    whole = exchange(mine, "grp")
    spread = exchange(packed(whole, shards, tiles), SHARD)
    new_first, new_second, update = slots(whole, hit, *rows)
    weights = (
        w_one,
        w_two,
        w_three,
        first_one,
        first_two,
        first_three,
        second_one,
        second_two,
        second_three,
    )
    new_table, *rest = last(slot_column, spread, rows[0], update, weights)
    back = [a.reshape(table.shape) for a in (new_table, new_first, new_second)]
    return (*back, *rest)


def solution(mesh):
    finer = Mesh(
        mesh.devices.reshape(mesh.shape["grp"], 4, 4, 2), ("grp", "shard_0", "shard_1", "shard_2")
    )
    rows = P(SHARD, None, None)
    placed = (
        rows,
        rows,
        rows,
        P(SHARD),
        P("grp", SHARD),
        P("grp", SHARD, None, None),
        P(),
        P(None, GRP_SHARD),
        P(GRP_SHARD, None),
    ) + (P(),) * 9
    return jax.shard_map(
        body,
        mesh=finer,
        in_specs=placed,
        out_specs=(rows, rows, rows) + (P(),) * 9,
        check_vma=False,
    )
```
